128 devices in a mesh: dp: 2 (over core), seq: 64 (over z, x, y).
Axes of the slice: x: 4, y: 4, z: 4, core: 2. Of those that a mesh axis runs over, the one named last changes fastest.
Arguments:
- queries: bfloat16 [2, 16384, 2048], P('dp', 'seq'), may hold values from -6 to 6
- keys: bfloat16 [2, 16384, 2048], P('dp', 'seq'), may hold values from -6 to 6
- values: bfloat16 [2, 16384, 2048], P('dp', 'seq'), may hold values from -6 to 6
- out_grad: bfloat16 [2, 16384, 4096], P('dp', 'seq'), may hold values from -6 to 6
- out_weight: bfloat16 [2048, 4096], replicated, may hold values from -0.125 to 0.125
Outputs:
- attended: bfloat16 [2, 16384, 2048], P('dp', 'seq')
- query_grad: bfloat16 [2, 16384, 2048], P('dp', 'seq')
- key_grad: bfloat16 [2, 16384, 2048], P('dp', 'seq')
- value_grad: bfloat16 [2, 16384, 2048], P('dp', 'seq')
- weight_grad: float32 [2048, 4096], P(('dp', 'seq'))
The draws below stay inside these ranges and needn't reach their ends.
All inputs are finite; a program needn't handle non-finite values.
Results may differ from the reference program's by a relative error of at most 0.0051.
Values sent between devices are 32-bit elements; how exact they have to be, the bound alone decides.
A program may use at most 192 MiB of HBM per device.

```python
import jax
import jax.numpy as jnp
from jax import lax

D = 4096
P_SIZE = 128
H = 16
TOK_DEV = 256
HD = 2048
LEN = 16384
SEQS = 2
N_SEQ = 64


def level_of(own_key, dims, pieces, smallest, high):
    def one(dim, parts):
        draws = jax.random.uniform(jax.random.fold_in(jax.random.fold_in(own_key, 6), dim), (parts,), jnp.float32, smallest / len(pieces), high / len(pieces))
        return jnp.repeat(jnp.exp(draws), dims[dim] // parts).reshape((-1,) + (1,) * (len(dims) - dim - 1))

    gain = one(*pieces[0])
    for cut in pieces[1:]:
        gain = gain * one(*cut)
    return gain


def noise(own_key, extent, width, bound, split=(), kind=jnp.bfloat16):
    values = width * jax.random.normal(own_key, extent, jnp.float32)
    if split:
        values = values * level_of(own_key, extent, split, -0.22, 0.18)
    return jnp.clip(values, -bound, bound).astype(kind)


def setup_inputs(seed: int = 0) -> dict:
    seeds = jax.random.split(jax.random.key(seed), 6)
    return {
        "queries": noise(seeds[0], (SEQS, LEN, HD), 1.0, 6.0, ((0, 2), (1, 64))),
        "keys": noise(seeds[1], (SEQS, LEN, HD), 1.0, 6.0, ((0, 2), (1, 64))),
        "values": noise(seeds[2], (SEQS, LEN, HD), 1.0, 6.0, ((0, 2), (1, 64))),
        "out_grad": noise(seeds[3], (SEQS, LEN, D), 1.0, 6.0, ((0, 2), (1, 64))),
        "out_weight": noise(seeds[4], (HD, D), HD ** -0.5, 0.125),
    }


EPS = 1e-06
HIGH = lax.Precision.HIGHEST

def span_forward(qf, kf, vf, prefix):
    count = qf.shape[0]
    scores = jnp.einsum('thp,shp->hts', qf, kf, precision=HIGH)
    lower = jnp.arange(count)[:, None] >= jnp.arange(count)[None, :]
    probs = jnp.where(lower[None], scores, 0.0).astype(jnp.bfloat16)
    intra = jnp.einsum('hts,shp->thp', probs.astype(jnp.float32), vf, precision=HIGH)
    inter = jnp.einsum('thp,hpe->the', qf, prefix, precision=HIGH)
    outputs = intra + inter
    inverse = lax.rsqrt(lax.optimization_barrier(jnp.mean(outputs * outputs, axis=-1, keepdims=True)) + EPS)
    return (outputs, inverse, probs)

def span_backward(qf, kf, vf, prefix, probs, d_out):
    count = qf.shape[0]
    dof = d_out.astype(jnp.float32)
    lower = jnp.arange(count)[:, None] >= jnp.arange(count)[None, :]
    d_scores = jnp.einsum('the,she->hts', dof, vf, precision=HIGH)
    d_probs = jnp.where(lower[None], d_scores, 0.0).astype(jnp.bfloat16).astype(jnp.float32)
    d_query = jnp.einsum('hts,shp->thp', d_probs, kf, precision=HIGH) + jnp.einsum('the,hpe->thp', dof, prefix, precision=HIGH)
    d_key = jnp.einsum('hts,thp->shp', d_probs, qf, precision=HIGH)
    d_value = jnp.einsum('hts,the->she', probs.astype(jnp.float32), dof, precision=HIGH)
    d_prefix = jnp.einsum('thp,the->hpe', qf, dof, precision=HIGH)
    return (d_query, d_key, d_value, d_prefix)

def one_sequence(queries, keys, values, out_grad, out_weight):
    shape = (N_SEQ, TOK_DEV, H, P_SIZE)
    qf = queries.reshape(shape).astype(jnp.float32)
    kf = keys.reshape(shape).astype(jnp.float32)
    vf = values.reshape(shape).astype(jnp.float32)
    states = jnp.einsum('cshp,cshe->chpe', kf, vf, precision=HIGH)
    running = jnp.cumsum(states, axis=0)
    prefix = jnp.concatenate([jnp.zeros_like(states[:1]), running[:-1]], axis=0)
    outputs, inverse, probs = jax.vmap(span_forward)(qf, kf, vf, prefix)
    normed = outputs * inverse
    attended = normed.astype(jnp.bfloat16)
    grad = jnp.dot(out_grad.astype(jnp.float32), out_weight.astype(jnp.float32).T, precision=HIGH).reshape(shape)
    d_out = (inverse * (grad - normed * lax.optimization_barrier(jnp.mean(grad * normed, axis=-1, keepdims=True)))).astype(jnp.bfloat16)
    d_query, d_key, d_value, d_prefix = jax.vmap(span_backward)(qf, kf, vf, prefix, probs, d_out)
    later = jnp.cumsum(d_prefix[::-1], axis=0)[::-1]
    suffix = jnp.concatenate([later[1:], jnp.zeros_like(later[:1])], axis=0)
    d_key = d_key + jnp.einsum('cshe,chpe->cshp', vf, suffix, precision=HIGH)
    d_value = d_value + jnp.einsum('cshp,chpe->cshe', kf, suffix, precision=HIGH)
    flat = (LEN, HD)
    return (attended.reshape(flat), d_query.astype(jnp.bfloat16).reshape(flat), d_key.astype(jnp.bfloat16).reshape(flat), d_value.astype(jnp.bfloat16).reshape(flat))

def reference(queries, keys, values, out_grad, out_weight):

    def apply(items):
        return one_sequence(items[0], items[1], items[2], items[3], out_weight)
    attended, query_grad, key_grad, value_grad = lax.map(apply, (queries, keys, values, out_grad))
    every = attended.reshape(SEQS * LEN, HD).astype(jnp.float32)
    cotangent = out_grad.reshape(SEQS * LEN, D).astype(jnp.float32)
    weight_grad = jnp.dot(every.T, cotangent, precision=HIGH)
    return (attended, query_grad, key_grad, value_grad, weight_grad)
```

```python
import functools

import jax
import jax.numpy as jnp
from jax import lax
from jax.experimental import pallas as pl
from jax.experimental.pallas import tpu as pltpu
from jax.sharding import Mesh
from jax.sharding import PartitionSpec as P

P_SIZE = 128
H = 16
HD = 2048
D = 4096
TOK = 256
EPS = 1e-06
F32 = jnp.float32
BF16 = jnp.bfloat16
MESH = pl.DeviceIdType.MESH
DP = "dp"
SEQ = ("seq_0", "seq_1", "seq_2")
DP_SEQ = (DP,) + SEQ
N_CHUNK = 4
WIDTHS = (1536, 1280, 1280)
STARTS = (0, 1536, 2816)
ORDERS = ((0, 1, 2), (1, 2, 0), (2, 0, 1))
COL = 256
W_ROWS = 256
W_TILES = HD // W_ROWS


def dot_nn(a, b):
    return lax.dot_general(a, b, (((1,), (0,)), ((), ())), preferred_element_type=F32)


def dot_nt(a, b):
    return lax.dot_general(a, b, (((1,), (1,)), ((), ())), preferred_element_type=F32)


def dot_tn(a, b):
    return lax.dot_general(a, b, (((0,), (0,)), ((), ())), preferred_element_type=F32)


def two_parts(x):
    high = x.astype(BF16)
    return high, (x - high.astype(F32)).astype(BF16)


def send(src, dst, send_sem, recv_sem, device):
    return pltpu.make_async_remote_copy(
        src_ref=src, dst_ref=dst, send_sem=send_sem, recv_sem=recv_sem,
        device_id=device, device_id_type=MESH,
    )


class Scan:
    def __init__(self, where, bufs, sems, reverse):
        self.z, self.x, self.y = where
        self.S, self.YR, self.T, self.XR, self.PT, self.ZR, self.XC, self.R = bufs
        self.ss, self.rs = sems
        self.reverse = reverse

    def order(self):
        return range(3, -1, -1) if self.reverse else range(4)

    def copies(self, stage, c):
        out = []
        for r in range(1, 4):
            s, v = self.ss.at[c, stage, r], self.rs.at[c, stage, r]
            yt, xt, zt = (self.y + r) % 4, (self.x + r) % 4, (self.z + r) % 4
            if stage == 0:
                out.append(send(self.S.at[yt, c], self.YR.at[c, self.y], s, v, {SEQ[2]: yt}))
            elif stage == 1:
                out.append(send(self.T.at[c, xt], self.XR.at[c, self.x], s, v, {SEQ[1]: xt}))
            elif stage == 2:
                out.append(send(self.PT.at[c], self.ZR.at[c, self.z], s, v, {SEQ[0]: zt}))
            elif stage == 3:
                out.append(send(self.XR.at[c, xt], self.XC.at[c, self.x], s, v, {SEQ[1]: xt}))
            else:
                out.append(send(self.YR.at[c, yt], self.R.at[self.y, c], s, v, {SEQ[2]: yt}))
        return out

    def landing(self, stage, c):
        for r in range(1, 4):
            s, v = self.ss.at[c, stage, r], self.rs.at[c, stage, r]
            yf, xf, zf = (self.y + 4 - r) % 4, (self.x + 4 - r) % 4, (self.z + 4 - r) % 4
            if stage == 0:
                ref, dev = self.YR.at[c, yf], {SEQ[2]: yf}
            elif stage == 1:
                ref, dev = self.XR.at[c, xf], {SEQ[1]: xf}
            elif stage == 2:
                ref, dev = self.ZR.at[c, zf], {SEQ[0]: zf}
            elif stage == 3:
                ref, dev = self.XC.at[c, xf], {SEQ[1]: xf}
            else:
                ref, dev = self.R.at[yf, c], {SEQ[2]: yf}
            send(ref, ref, s, v, dev).wait_recv()

    def go(self, stage, c):
        for copy in self.copies(stage, c):
            copy.start()

    def step(self, s, c):
        if s > 0:
            self.landing(s - 1, c)
        if s == 0:
            self.YR[c, self.y] = self.S[self.y, c]
        elif s == 1:
            running = None
            for k in self.order():
                now = self.YR[c, k]
                self.YR[c, k] = jnp.zeros_like(now) if running is None else running
                running = now if running is None else running + now
            self.T[c] = running.reshape(4, 32, 128)
            self.XR[c, self.x] = self.T[c, self.x]
        elif s == 2:
            running = None
            for k in self.order():
                now = self.XR[c, k]
                self.XR[c, k] = jnp.zeros_like(now) if running is None else running
                running = now if running is None else running + now
            self.PT[c] = running
            self.ZR[c, self.z] = running
        elif s == 3:
            base = jnp.zeros((32, 128), F32)
            for k in range(4):
                passed = (self.z < k) if self.reverse else (self.z > k)
                base = base + jnp.where(passed, self.ZR[c, k], 0.0)
            for k in range(4):
                self.XR[c, k] = self.XR[c, k] + base
            self.XC[c, self.x] = self.XR[c, self.x]
        elif s == 4:
            carry = self.XC[c].reshape(128, 128)
            for k in range(4):
                self.YR[c, k] = self.YR[c, k] + carry
            self.R[self.y, c] = self.YR[c, self.y]
        if s < 5:
            self.go(s, c)

    def drain(self, stage):
        for c in range(N_CHUNK):
            for copy in self.copies(stage, c):
                copy.wait_send()


class Color:
    def __init__(self, where, order, part, recv, ss, rs):
        self.where, self.order, self.part, self.recv, self.ss, self.rs = where, order, part, recv, ss, rs

    def axis(self, phase):
        return self.order[phase]

    def slot(self, phase, t, u):
        idx = [slice(None)] * 3
        for p in range(phase):
            idx[self.order[p]] = self.where[self.order[p]]
        idx[self.order[phase]] = t
        if phase == 0:
            nxt = self.order[1]
            idx[nxt] = (self.where[nxt] + (2, 1, 3, 0)[u]) % 4
        return idx

    def number(self, phase, kind, u):
        return (kind * 4 + u) if phase == 0 else (24 + 6 * (phase - 1) + kind)

    def copy(self, phase, kind, u=0):
        a = self.axis(phase)
        m = self.where[a]
        up = kind % 2 == 0
        to = (m + 1) % 4 if up else (m + 3) % 4
        t = (m + 2) % 4 if kind < 2 else to
        half = (0, 1, 1, 0, 0, 1)[kind]
        n = self.number(phase, kind, u)
        src = self.part.at[tuple(self.slot(phase, t, u)) + (half,)]
        dst = self.recv[phase].at[kind, u] if phase == 0 else self.recv[phase].at[kind]
        return send(src, dst, self.ss.at[n], self.rs.at[n], {SEQ[a]: to})

    def go(self, phase, kind, u=0):
        self.copy(phase, kind, u).start()

    def got(self, phase, kind, u=0):
        self.copy(phase, kind, u).wait_recv()
        return self.recv[phase][kind, u] if phase == 0 else self.recv[phase][kind]

    def relay(self, phase, u=0):
        m = self.where[self.axis(phase)]
        for kind, to, half in ((0, (m + 1) % 4, 0), (1, (m + 3) % 4, 1)):
            more = self.got(phase, kind, u)
            at = tuple(self.slot(phase, to, u)) + (half,)
            self.part[at] = self.part[at] + more
            self.go(phase, 4 + kind, u)

    def finish(self, phase, u=0):
        m = self.where[self.axis(phase)]
        for half, kinds in ((0, (3, 4)), (1, (2, 5))):
            more = self.got(phase, kinds[0], u) + self.got(phase, kinds[1], u)
            at = tuple(self.slot(phase, m, u)) + (half,)
            self.part[at] = self.part[at] + more

    def drain(self):
        for kind in range(6):
            for u in range(4):
                self.copy(0, kind, u).wait_send()
            for phase in (1, 2):
                self.copy(phase, kind).wait_send()


def kernel(
    q_hbm, k_hbm, v_hbm, og_hbm, w_hbm,
    att_out, qg_out, kg_out, vg_out, wg_out,
    q_v, k_v, v_v, og_v, ogp_v, w_v, grad_v, att_v, do_v, attT, attP, attS, attR,
    state, yr1, t1, xr1, pt1, zr1, xc1, r1,
    yr2, t2, xr2, pt2, zr2, xc2, r2,
    p0, p1, p2, a0, a1, a2, b0, b1, b2, c0, c1, c2,
    in_sem, w_sem, out_sem, s1s, s1r, s2s, s2r, css, crs, ogs, ogr, ats, atr,
):
    d = lax.axis_index(DP)
    where = tuple(lax.axis_index(a) for a in SEQ)
    z, x, y = where
    other = {DP: 1 - d}
    parts = (p0, p1, p2)

    loads = [
        pltpu.make_async_copy(src.at[0], dst, in_sem.at[i])
        for i, (src, dst) in enumerate(((k_hbm, k_v), (v_hbm, v_v), (og_hbm, og_v), (q_hbm, q_v)))
    ]
    for load in loads:
        load.start()

    def w_load(i):
        return pltpu.make_async_copy(
            w_hbm.at[pl.ds(pl.multiple_of(i * W_ROWS, W_ROWS), W_ROWS)], w_v.at[i % 2], w_sem.at[i % 2]
        )

    w_load(0).start()
    w_load(1).start()

    barrier = pltpu.get_barrier_semaphore()
    pl.semaphore_signal(barrier, inc=1, device_id=other, device_id_type=MESH)
    for a in range(3):
        for r in range(1, 4):
            pl.semaphore_signal(barrier, inc=1, device_id={SEQ[a]: (where[a] + r) % 4}, device_id_type=MESH)

    scan1 = Scan(where, (state, yr1, t1, xr1, pt1, zr1, xc1, r1), (s1s, s1r), False)
    scan2 = Scan(where, (state, yr2, t2, xr2, pt2, zr2, xc2, r2), (s2s, s2r), True)
    colors = [
        Color(where, ORDERS[i], parts[i], ((a0, b0, c0), (a1, b1, c1), (a2, b2, c2))[i], css.at[i], crs.at[i])
        for i in range(3)
    ]

    def cols(h):
        return pl.ds(pl.multiple_of(h * P_SIZE, P_SIZE), P_SIZE)

    def states(c):
        def one(j, carry):
            at = cols(4 * j + c)
            state[j, c] = dot_tn(k_v[:, at], v_v[:, at])
            return carry
        lax.fori_loop(0, 4, one, 0)

    loads[0].wait()
    loads[1].wait()
    states(0)
    pl.semaphore_wait(barrier, 10)
    scan1.step(0, 0)
    for c in range(1, N_CHUNK):
        states(c)
        scan1.step(0, c)

    loads[2].wait()

    def og_copy(i):
        return send(parts[i].at[0], parts[i].at[1], ogs.at[i], ogr.at[i], other)

    for i in range(3):
        def put(n, carry, i=i):
            rows = pl.ds(pl.multiple_of(n * 64, 64), 64)
            block = og_v[rows, STARTS[i]:STARTS[i] + WIDTHS[i]].astype(F32)
            parts[i][0, n] = block.reshape(4, 2, 8, WIDTHS[i])
            return carry
        lax.fori_loop(0, 4, put, 0)
        og_copy(i).start()

    def grad_tiles(lo, hi):
        def one(i, carry):
            w_load(i).wait()
            block = dot_nt(og_v[...], w_v[i % 2])
            at = pl.ds(pl.multiple_of(i * W_ROWS, W_ROWS), W_ROWS)
            grad_v[:, at] = block

            @pl.when(i + 2 < W_TILES)
            def _():
                w_load(i + 2).start()
            return carry
        lax.fori_loop(lo, hi, one, 0)

    def og_take(i):
        og_copy(i).wait_recv()
        def take(n, carry):
            rows = pl.ds(pl.multiple_of(n * 64, 64), 64)
            block = parts[i][1, n].reshape(64, WIDTHS[i])
            ogp_v[rows, STARTS[i]:STARTS[i] + WIDTHS[i]] = block.astype(BF16)
            return carry
        lax.fori_loop(0, 4, take, 0)

    lower = (
        lax.broadcasted_iota(jnp.int32, (TOK, TOK), 0) >= lax.broadcasted_iota(jnp.int32, (TOK, TOK), 1)
    )

    def forward_heads(c):
        def one(j, carry):
            h = 4 * j + c
            at = cols(h)
            q, k, v = q_v[:, at], k_v[:, at], v_v[:, at]
            probs = jnp.where(lower, dot_nt(q, k), 0.0).astype(BF16)
            high, low = two_parts(r1[j, c])
            o = dot_nn(probs, v) + (dot_nn(q, high) + dot_nn(q, low))
            inverse = lax.rsqrt(jnp.mean(o * o, axis=-1, keepdims=True) + EPS)
            a = o * inverse
            att = a.astype(BF16)
            att_v[:, at] = att
            turned = att.astype(F32).T.astype(BF16).reshape(2, 4, 16, TOK)
            hh = h % 8
            attT[h // 8, hh // 2, pl.ds(2 * (hh % 2), 2)] = turned
            grad = grad_v[:, at]
            d_o = (inverse * (grad - a * jnp.mean(grad * a, axis=-1, keepdims=True))).astype(BF16)
            do_v[:, at] = d_o
            state[j, c] = dot_tn(q, d_o)
            return carry
        lax.fori_loop(0, 4, one, 0)

    def att_copies(c):
        return [
            send(attS.at[2 * c + i], attR.at[2 * c + i], ats.at[2 * c + i], atr.at[2 * c + i], other)
            for i in range(2)
        ]

    def att_give(c):
        for i, copy in enumerate(att_copies(c)):
            hh = 4 * i + c
            attS[2 * c + i] = attT[1 - d, hh // 2, 2 * (hh % 2):2 * (hh % 2) + 2].astype(F32)
            copy.start()

    def att_take(c):
        for i, copy in enumerate(att_copies(c)):
            hh = 4 * i + c
            copy.wait_recv()
            attP[hh // 2, 2 * (hh % 2):2 * (hh % 2) + 2] = attR[2 * c + i].astype(BF16)

    grad_tiles(0, 4)
    fill = {1: lambda: grad_tiles(4, 6), 2: lambda: grad_tiles(6, 8), 3: lambda: og_take(0),
            4: lambda: og_take(1), 5: lambda: og_take(2)}
    for t in range(1, 5 + N_CHUNK):
        for s in range(5, 0, -1):
            c = t - s
            if 0 <= c < N_CHUNK:
                scan1.step(s, c)
                if s == 5:
                    if c == 0:
                        scan1.drain(0)
                        loads[3].wait()
                    forward_heads(c)
                    scan2.step(0, c)
                    att_give(c)
        if t in fill:
            fill[t]()
    att_save = pltpu.make_async_copy(att_v, att_out.at[0], out_sem.at[0])
    att_save.start()
    for c in range(N_CHUNK):
        att_take(c)
    for i in range(3):
        og_copy(i).wait_send()

    def product(i, offset):
        color = colors[i]
        axis = ORDERS[i][0]
        t = (where[axis] + offset) % 4
        idx = [slice(None)] * 3
        idx[axis] = t
        idx = tuple(idx)
        mine = attT[(d,) + idx].reshape(TOK, TOK)
        theirs = attP[idx].reshape(TOK, TOK)

        def one(n, carry):
            at = pl.ds(pl.multiple_of(STARTS[i] + n * COL, COL), COL)
            block = dot_nn(mine, og_v[:, at]) + dot_nn(theirs, ogp_v[:, at])
            to = pl.ds(pl.multiple_of(n * COL, COL), COL)
            color.part[idx + (slice(None), slice(None), to)] = block.reshape(4, 4, 2, 8, COL)
            return carry
        lax.fori_loop(0, WIDTHS[i] // COL, one, 0)

    def backward_heads(c):
        def one(j, carry):
            at = cols(4 * j + c)
            q, k, v, d_o = q_v[:, at], k_v[:, at], v_v[:, at], do_v[:, at]
            probs = jnp.where(lower, dot_nt(q, k), 0.0).astype(BF16)
            d_probs = jnp.where(lower, dot_nt(d_o, v), 0.0).astype(BF16)
            high, low = two_parts(r1[j, c])
            q_grad = dot_nn(d_probs, k) + (dot_nt(d_o, high) + dot_nt(d_o, low))
            high, low = two_parts(r2[j, c])
            k_grad = dot_tn(d_probs, q) + (dot_nt(v, high) + dot_nt(v, low))
            v_grad = dot_tn(probs, d_o) + (dot_nn(k, high) + dot_nn(k, low))
            q_v[:, at] = q_grad.astype(BF16)
            k_v[:, at] = k_grad.astype(BF16)
            v_v[:, at] = v_grad.astype(BF16)
            return carry
        lax.fori_loop(0, 4, one, 0)

    for i in range(3):
        product(i, 2)
        for u in range(4):
            colors[i].go(0, 0, u)
            colors[i].go(0, 1, u)
    for i in range(3):
        product(i, 1)
        for u in range(4):
            colors[i].go(0, 2, u)
    for i in range(3):
        product(i, 3)
        for u in range(4):
            colors[i].go(0, 3, u)
    for i in range(3):
        product(i, 0)

    for t in range(1, 5 + N_CHUNK):
        for s in range(5, 0, -1):
            c = t - s
            if 0 <= c < N_CHUNK:
                scan2.step(s, c)
                if s == 5:
                    backward_heads(c)
        if t <= 4:
            for color in colors:
                color.relay(0, t - 1)
    saves = [
        pltpu.make_async_copy(src, dst.at[0], out_sem.at[1 + i])
        for i, (src, dst) in enumerate(((q_v, qg_out), (k_v, kg_out), (v_v, vg_out)))
    ]
    for save in saves:
        save.start()

    for u in range(4):
        for color in colors:
            color.finish(0, u)
            if u == 0:
                color.go(1, 0)
                color.go(1, 1)
            elif u == 1:
                color.go(1, 2)
            elif u == 2:
                color.go(1, 3)
    for color in colors:
        color.relay(1)
    for color in colors:
        color.finish(1)
        for kind in range(4):
            color.go(2, kind)
    for color in colors:
        color.relay(2)
    outs = []
    for i, color in enumerate(colors):
        color.finish(2)
        out = pltpu.make_async_copy(
            color.part.at[z, x, y],
            wg_out.at[:, :, STARTS[i]:STARTS[i] + WIDTHS[i]],
            out_sem.at[4 + i],
        )
        out.start()
        outs.append(out)

    for stage in range(1, 5):
        scan1.drain(stage)
    for stage in range(5):
        scan2.drain(stage)
    for color in colors:
        color.drain()
    for c in range(N_CHUNK):
        for copy in att_copies(c):
            copy.wait_send()
    att_save.wait()
    for save in saves:
        save.wait()
    for out in outs:
        out.wait()


def body(queries, keys, values, out_grad, out_weight):
    vm = pltpu.VMEM
    dma = pltpu.SemaphoreType.DMA
    flat = jax.ShapeDtypeStruct((1, TOK, HD), BF16)

    def scan_bufs():
        return [
            vm((4, 4, 128, 128), F32), vm((4, 4, 32, 128), F32), vm((4, 4, 32, 128), F32),
            vm((4, 32, 128), F32), vm((4, 4, 32, 128), F32), vm((4, 4, 32, 128), F32),
            vm((4, 4, 128, 128), F32),
        ]

    scratch = [
        vm((TOK, HD), BF16), vm((TOK, HD), BF16), vm((TOK, HD), BF16),
        vm((TOK, D), BF16), vm((TOK, D), BF16), vm((2, W_ROWS, D), BF16),
        vm((TOK, HD), F32), vm((TOK, HD), BF16), vm((TOK, HD), BF16),
        vm((2, 4, 4, 4, 16, TOK), BF16), vm((4, 4, 4, 16, TOK), BF16),
        vm((8, 2, 4, 16, TOK), F32), vm((8, 2, 4, 16, TOK), F32),
        vm((4, 4, 128, 128), F32),
        *scan_bufs(), *scan_bufs(),
        *[vm((4, 4, 4, 2, 8, w), F32) for w in WIDTHS],
    ]
    scratch += [vm((6, 4, 4, 8, w), F32) for w in WIDTHS]
    scratch += [vm((6, 4, 8, w), F32) for w in WIDTHS]
    scratch += [vm((6, 8, w), F32) for w in WIDTHS]
    scratch += [
        dma((4,)), dma((2,)), dma((7,)),
        dma((4, 5, 4)), dma((4, 5, 4)), dma((4, 5, 4)), dma((4, 5, 4)),
        dma((3, 36)), dma((3, 36)), dma((3,)), dma((3,)), dma((8,)), dma((8,)),
    ]
    any_space = pl.BlockSpec(memory_space=pl.ANY)
    attended, d_query, d_key, d_value, weight_grad = pl.pallas_call(
        kernel,
        out_shape=(flat, flat, flat, flat, jax.ShapeDtypeStruct((2, 8, D), F32)),
        in_specs=[any_space] * 5,
        out_specs=(any_space,) * 5,
        scratch_shapes=scratch,
        compiler_params=pltpu.CompilerParams(
            collective_id=0, has_side_effects=True, vmem_limit_bytes=66_900_000
        ),
        name="block",
    )(queries, keys, values, out_grad, out_weight)
    return attended, d_query, d_key, d_value, weight_grad.reshape(16, D)


def solution(mesh):
    split = Mesh(mesh.devices.reshape(mesh.shape[DP], 4, 4, 4), DP_SEQ)
    rows = P(DP, SEQ, None)
    return jax.shard_map(
        body, mesh=split, in_specs=(rows, rows, rows, rows, P()),
        out_specs=(rows, rows, rows, rows, P(DP_SEQ, None)), check_vma=False,
    )
```

```python
import functools

import jax
import jax.numpy as jnp
from jax import lax
from jax.experimental import pallas as pl
from jax.experimental.pallas import tpu as pltpu
from jax.sharding import Mesh
from jax.sharding import PartitionSpec as P

P_SIZE = 128
H = 16
HD = 2048
D = 4096
TOK = 256
EPS = 1e-06
F32 = jnp.float32
BF16 = jnp.bfloat16
MESH = pl.DeviceIdType.MESH
DP = "dp"
SEQ = ("seq_0", "seq_1", "seq_2")
DP_SEQ = (DP,) + SEQ
N_CHUNK = 4
WIDTHS = (1536, 1280, 1280)
STARTS = (0, 1536, 2816)
ORDERS = ((0, 1, 2), (1, 2, 0), (2, 0, 1))
COL = 256
W_ROWS = 256
W_TILES = HD // W_ROWS
VMEM_LIMIT = 62_000_000


def dot_nn(a, b):
    return lax.dot_general(a, b, (((1,), (0,)), ((), ())), preferred_element_type=F32)


def dot_nt(a, b):
    return lax.dot_general(a, b, (((1,), (1,)), ((), ())), preferred_element_type=F32)


def dot_tn(a, b):
    return lax.dot_general(a, b, (((0,), (0,)), ((), ())), preferred_element_type=F32)


def two_parts(x):
    high = x.astype(BF16)
    return high, (x - high.astype(F32)).astype(BF16)


def send(src, dst, send_sem, recv_sem, device):
    return pltpu.make_async_remote_copy(
        src_ref=src, dst_ref=dst, send_sem=send_sem, recv_sem=recv_sem,
        device_id=device, device_id_type=MESH,
    )


def scoped(f):
    @functools.wraps(f)
    def named(*args):
        with jax.named_scope(f.__name__ + "_" + "".join(map(str, args))):
            return f(*args)
    return named


class Scan:
    def __init__(self, where, bufs, sems, reverse):
        self.z, self.x, self.y = where
        self.S, self.YR, self.T, self.XR, self.PT, self.ZR, self.XC, self.R = bufs
        self.ss, self.rs = sems
        self.reverse = reverse

    def order(self):
        return range(3, -1, -1) if self.reverse else range(4)

    def copies(self, stage, c):
        out = []
        for r in range(1, 4):
            s, v = self.ss.at[c, stage, r], self.rs.at[c, stage, r]
            yt, xt, zt = (self.y + r) % 4, (self.x + r) % 4, (self.z + r) % 4
            if stage == 0:
                out.append(send(self.S.at[yt, c], self.YR.at[c, self.y], s, v, {SEQ[2]: yt}))
            elif stage == 1:
                out.append(send(self.T.at[c, xt], self.XR.at[c, self.x], s, v, {SEQ[1]: xt}))
            elif stage == 2:
                out.append(send(self.PT.at[c], self.ZR.at[c, self.z], s, v, {SEQ[0]: zt}))
            elif stage == 3:
                out.append(send(self.XR.at[c, xt], self.XC.at[c, self.x], s, v, {SEQ[1]: xt}))
            else:
                out.append(send(self.YR.at[c, yt], self.R.at[self.y, c], s, v, {SEQ[2]: yt}))
        return out

    def landing(self, stage, c):
        for r in range(1, 4):
            s, v = self.ss.at[c, stage, r], self.rs.at[c, stage, r]
            yf, xf, zf = (self.y + 4 - r) % 4, (self.x + 4 - r) % 4, (self.z + 4 - r) % 4
            if stage == 0:
                ref, dev = self.YR.at[c, yf], {SEQ[2]: yf}
            elif stage == 1:
                ref, dev = self.XR.at[c, xf], {SEQ[1]: xf}
            elif stage == 2:
                ref, dev = self.ZR.at[c, zf], {SEQ[0]: zf}
            elif stage == 3:
                ref, dev = self.XC.at[c, xf], {SEQ[1]: xf}
            else:
                ref, dev = self.R.at[yf, c], {SEQ[2]: yf}
            send(ref, ref, s, v, dev).wait_recv()

    def go(self, stage, c):
        for copy in self.copies(stage, c):
            copy.start()

    def step(self, s, c):
        with jax.named_scope(f"scan{int(self.reverse)}_{s}{c}"):
            self.step_in(s, c)

    def step_in(self, s, c):
        if s > 0:
            self.landing(s - 1, c)
        if s == 0:
            self.YR[c, self.y] = self.S[self.y, c]
        elif s == 1:
            running = None
            for k in self.order():
                now = self.YR[c, k]
                self.YR[c, k] = jnp.zeros_like(now) if running is None else running
                running = now if running is None else running + now
            self.T[c] = running.reshape(4, 32, 128)
            self.XR[c, self.x] = self.T[c, self.x]
        elif s == 2:
            running = None
            for k in self.order():
                now = self.XR[c, k]
                self.XR[c, k] = jnp.zeros_like(now) if running is None else running
                running = now if running is None else running + now
            self.PT[c] = running
            self.ZR[c, self.z] = running
        elif s == 3:
            base = jnp.zeros((32, 128), F32)
            for k in range(4):
                passed = (self.z < k) if self.reverse else (self.z > k)
                base = base + jnp.where(passed, self.ZR[c, k], 0.0)
            for k in range(4):
                self.XR[c, k] = self.XR[c, k] + base
            self.XC[c, self.x] = self.XR[c, self.x]
        elif s == 4:
            carry = self.XC[c].reshape(128, 128)
            for k in range(4):
                self.YR[c, k] = self.YR[c, k] + carry
            self.R[self.y, c] = self.YR[c, self.y]
        if s < 5:
            self.go(s, c)

    def drain(self, stage):
        for c in range(N_CHUNK):
            for copy in self.copies(stage, c):
                copy.wait_send()


class Color:
    def __init__(self, where, order, part, recv, ss, rs):
        self.where, self.order, self.part, self.recv, self.ss, self.rs = where, order, part, recv, ss, rs
        self.gone = set()

    def axis(self, phase):
        return self.order[phase]

    def slot(self, phase, t, u):
        idx = [slice(None)] * 3
        for p in range(phase):
            idx[self.order[p]] = self.where[self.order[p]]
        idx[self.order[phase]] = t
        if phase == 0:
            nxt = self.order[1]
            idx[nxt] = (self.where[nxt] + (2, 1, 3, 0)[u]) % 4
        return idx

    def number(self, phase, kind, u):
        return (kind * 4 + u) if phase == 0 else (24 + 6 * (phase - 1) + kind)

    def copy(self, phase, kind, u=0):
        a = self.axis(phase)
        m = self.where[a]
        up = kind % 2 == 0
        to = (m + 1) % 4 if up else (m + 3) % 4
        t = (m + 2) % 4 if kind < 2 else to
        half = (0, 1, 1, 0, 0, 1)[kind]
        n = self.number(phase, kind, u)
        src = self.part.at[tuple(self.slot(phase, t, u)) + (half,)]
        dst = self.recv[phase].at[kind, u] if phase == 0 else self.recv[phase].at[kind]
        return send(src, dst, self.ss.at[n], self.rs.at[n], {SEQ[a]: to})

    def go(self, phase, kind, u=0):
        self.copy(phase, kind, u).start()

    def left(self, phase, kind, u=0):
        if (phase, kind, u) not in self.gone:
            self.gone.add((phase, kind, u))
            self.copy(phase, kind, u).wait_send()

    def got(self, phase, kind, u=0):
        self.copy(phase, kind, u).wait_recv()
        return self.recv[phase][kind, u] if phase == 0 else self.recv[phase][kind]

    def relay(self, phase, u=0):
        with jax.named_scope(f"relay{self.order[0]}_{phase}{u}"):
            self.relay_in(phase, u)

    def relay_in(self, phase, u=0):
        m = self.where[self.axis(phase)]
        for kind, to, half in ((0, (m + 1) % 4, 0), (1, (m + 3) % 4, 1)):
            more = self.got(phase, kind, u)
            at = tuple(self.slot(phase, to, u)) + (half,)
            self.part[at] = self.part[at] + more
            self.go(phase, 4 + kind, u)

    def finish(self, phase, u=0, to=None):
        with jax.named_scope(f"finish{self.order[0]}_{phase}{u}"):
            self.finish_in(phase, u, to)

    def finish_in(self, phase, u=0, to=None):
        m = self.where[self.axis(phase)]
        for half, kinds in ((0, (3, 4)), (1, (2, 5))):
            more = self.got(phase, kinds[0], u) + self.got(phase, kinds[1], u)
            at = tuple(self.slot(phase, m, u)) + (half,)
            if to is None:
                self.part[at] = self.part[at] + more
            else:
                out, start, width = to
                out[half, :, start:start + width] = self.part[at] + more

    def drain(self):
        for kind in range(6):
            for u in range(4):
                self.left(0, kind, u)
            for phase in (1, 2):
                self.left(phase, kind)


def kernel(
    q_hbm, k_hbm, v_hbm, og_hbm, w_hbm,
    att_v, q_v, k_v, v_v, wg_v,
    og_v, w_v, grad_v, intra_v, do_v, attT, attP, attS, attR,
    state, yr1, t1, xr1, pt1, zr1, xc1, r1,
    yr2, t2, xr2, pt2, zr2, xc2, r2,
    p0, p1, p2, a0, a1, a2, b0, b1, b2, c0, c1, c2,
    in_sem, w_sem, s1s, s1r, s2s, s2r, css, crs, ogs, ogr, ats, atr,
):
    d = lax.axis_index(DP)
    where = tuple(lax.axis_index(a) for a in SEQ)
    z, x, y = where
    other = {DP: 1 - d}
    parts = (p0, p1, p2)

    loads = [
        pltpu.make_async_copy(src.at[0], dst, in_sem.at[i])
        for i, (src, dst) in enumerate(((k_hbm, k_v), (v_hbm, v_v), (og_hbm, og_v.at[:TOK]), (q_hbm, q_v)))
    ]
    for load in loads:
        load.start()

    def w_load(i):
        return pltpu.make_async_copy(
            w_hbm.at[pl.ds(pl.multiple_of(i * W_ROWS, W_ROWS), W_ROWS)], w_v.at[i % 2], w_sem.at[i % 2]
        )

    w_load(0).start()
    w_load(1).start()

    barrier = pltpu.get_barrier_semaphore()
    pl.semaphore_signal(barrier, inc=1, device_id=other, device_id_type=MESH)
    for a in range(3):
        for r in range(1, 4):
            pl.semaphore_signal(barrier, inc=1, device_id={SEQ[a]: (where[a] + r) % 4}, device_id_type=MESH)

    scan1 = Scan(where, (state, yr1, t1, xr1, pt1, zr1, xc1, r1), (s1s, s1r), False)
    scan2 = Scan(where, (state, yr2, t2, xr2, pt2, zr2, xc2, r2), (s2s, s2r), True)
    colors = [
        Color(where, ORDERS[i], parts[i], ((a0, b0, c0), (a1, b1, c1), (a2, b2, c2))[i], css.at[i], crs.at[i])
        for i in range(3)
    ]

    def cols(h):
        return pl.ds(pl.multiple_of(h * P_SIZE, P_SIZE), P_SIZE)

    def heads_of(fn, c, width=2):
        def one(n, carry):
            fn([n * width + i for i in range(width)], c)
            return carry
        lax.fori_loop(0, 4 // width, one, 0)

    @scoped
    def states(c):
        def some(js, c):
            at = [cols(4 * j + c) for j in js]
            out = [dot_tn(k_v[:, a], v_v[:, a]) for a in at]
            for j, value in zip(js, out):
                state[j, c] = value
        heads_of(some, c)

    with jax.named_scope("load"):
        loads[0].wait()
        loads[1].wait()
    states(0)
    with jax.named_scope("enter"):
        pl.semaphore_wait(barrier, 10)
    scan1.step(0, 0)
    for c in range(1, N_CHUNK):
        states(c)
        scan1.step(0, c)

    loads[2].wait()

    def og_copy(i):
        return send(parts[i].at[0], parts[i].at[1], ogs.at[i], ogr.at[i], other)

    for i in range(3):
        def put(n, carry, i=i):
            rows = pl.ds(pl.multiple_of(n * 64, 64), 64)
            block = og_v[rows, STARTS[i]:STARTS[i] + WIDTHS[i]].astype(F32)
            parts[i][0, n] = block.reshape(4, 2, 8, WIDTHS[i])
            return carry
        lax.fori_loop(0, 4, put, 0)
        og_copy(i).start()

    @scoped
    def grad_tiles(lo, hi):
        def one(i, carry):
            w_load(i).wait()
            block = dot_nt(og_v[:TOK], w_v[i % 2])
            at = pl.ds(pl.multiple_of(i * W_ROWS, W_ROWS), W_ROWS)
            grad_v[:, at] = block

            @pl.when(i + 2 < W_TILES)
            def _():
                w_load(i + 2).start()
            return carry
        lax.fori_loop(lo, hi, one, 0)

    @scoped
    def og_take(i):
        og_copy(i).wait_recv()
        def take(n, carry):
            rows = pl.ds(pl.multiple_of(TOK + n * 64, 64), 64)
            block = parts[i][1, n].reshape(64, WIDTHS[i])
            og_v[rows, STARTS[i]:STARTS[i] + WIDTHS[i]] = block.astype(BF16)
            return carry
        lax.fori_loop(0, 4, take, 0)

    lower = (
        lax.broadcasted_iota(jnp.int32, (TOK, TOK), 0) >= lax.broadcasted_iota(jnp.int32, (TOK, TOK), 1)
    )

    @scoped
    def inside_heads(c):
        def some(js, c):
            at = [cols(4 * j + c) for j in js]
            scores = [dot_nt(q_v[:, a], k_v[:, a]) for a in at]
            probs = [jnp.where(lower, x, 0.0).astype(BF16) for x in scores]
            out = [dot_nn(p, v_v[:, a]) for p, a in zip(probs, at)]
            for a, value in zip(at, out):
                intra_v[:, a] = value
        heads_of(some, c)

    @scoped
    def forward_heads(c):
        def some(js, c):
            at = [cols(4 * j + c) for j in js]
            q = [q_v[:, a] for a in at]
            split = [two_parts(r1[j, c]) for j in js]
            inter = [dot_nn(a, high) + dot_nn(a, low) for a, (high, low) in zip(q, split)]
            o = [intra_v[:, a] + x for a, x in zip(at, inter)]
            inverse = [lax.rsqrt(jnp.mean(x * x, axis=-1, keepdims=True) + EPS) for x in o]
            normed = [x * i for x, i in zip(o, inverse)]
            grad = [grad_v[:, a] for a in at]
            level = [jnp.mean(g * n, axis=-1, keepdims=True) for g, n in zip(grad, normed)]
            d_o = [(i * (g - n * m)).astype(BF16) for i, g, n, m in zip(inverse, grad, normed, level)]
            d_prefix = [dot_tn(a, b) for a, b in zip(q, d_o)]
            att = [n.astype(BF16) for n in normed]
            turned = [a.astype(F32).T.astype(BF16).reshape(2, 4, 16, TOK) for a in att]
            for i, j in enumerate(js):
                h = 4 * j + c
                hh = h % 8
                att_v[:, at[i]] = att[i]
                do_v[:, at[i]] = d_o[i]
                state[j, c] = d_prefix[i]
                attT[h // 8, hh // 2, pl.ds(2 * (hh % 2), 2)] = turned[i]
        heads_of(some, c)

    def att_copies(c):
        return [
            send(attS.at[2 * c + i], attR.at[2 * c + i], ats.at[2 * c + i], atr.at[2 * c + i], other)
            for i in range(2)
        ]

    @scoped
    def att_give(c):
        for i, copy in enumerate(att_copies(c)):
            hh = 4 * i + c
            attS[2 * c + i] = attT[1 - d, hh // 2, 2 * (hh % 2):2 * (hh % 2) + 2].astype(F32)
            copy.start()

    @scoped
    def att_take(c):
        for i, copy in enumerate(att_copies(c)):
            hh = 4 * i + c
            copy.wait_recv()
            attP[hh // 2, 2 * (hh % 2):2 * (hh % 2) + 2] = attR[2 * c + i].astype(BF16)

    forward = (
        (grad_tiles, 0, 4), (1, 0), (grad_tiles, 4, 6), (1, 1), (grad_tiles, 6, 8), (2, 0), (1, 2),
        (inside_heads, 0), (2, 1), (1, 3), (inside_heads, 1), (3, 0), (2, 2), (og_take, 0), (inside_heads, 2),
        (3, 1), (2, 3), (4, 0), (inside_heads, 3), (3, 2), (4, 1), (3, 3), (og_take, 1), (4, 2), (og_take, 2),
        (4, 3),
    )
    loads[3].wait()
    for item in forward:
        if callable(item[0]):
            item[0](*item[1:])
        else:
            scan1.step(*item)
    scan1.drain(0)
    for c in range(N_CHUNK):
        scan1.step(5, c)
        forward_heads(c)
        scan2.step(0, c)
        att_give(c)
        if c >= 2:
            scan2.step(1, c - 2)
    for c in range(N_CHUNK):
        att_take(c)
    for i in range(3):
        og_copy(i).wait_send()

    @scoped
    def product(i, offset):
        color = colors[i]
        axis = ORDERS[i][0]
        t = (where[axis] + offset) % 4
        idx = [slice(None)] * 3
        idx[axis] = t
        idx = tuple(idx)
        both = jnp.concatenate([attT[(d,) + idx].reshape(TOK, TOK), attP[idx].reshape(TOK, TOK)], axis=1)
        for n in range(WIDTHS[i] // COL):
            at = STARTS[i] + n * COL
            block = dot_nn(both, og_v[:, at:at + COL])
            color.part[idx + (slice(None), slice(None), slice(n * COL, (n + 1) * COL))] = block.reshape(4, 4, 2, 8, COL)

    @scoped
    def backward_heads(c):
        def some(js, c):
            at = [cols(4 * j + c) for j in js]
            q, k, v, d_o = ([ref[:, a] for a in at] for ref in (q_v, k_v, v_v, do_v))
            probs = [jnp.where(lower, dot_nt(a, b), 0.0).astype(BF16) for a, b in zip(q, k)]
            d_probs = [jnp.where(lower, dot_nt(a, b), 0.0).astype(BF16) for a, b in zip(d_o, v)]
            before = [two_parts(r1[j, c]) for j in js]
            after = [two_parts(r2[j, c]) for j in js]
            n = range(len(js))
            q_grad = [dot_nn(d_probs[i], k[i]) + sum(dot_nt(d_o[i], p) for p in before[i]) for i in n]
            k_grad = [dot_tn(d_probs[i], q[i]) + sum(dot_nt(v[i], p) for p in after[i]) for i in n]
            v_grad = [dot_tn(probs[i], d_o[i]) + sum(dot_nn(k[i], p) for p in after[i]) for i in n]
            for i in n:
                q_v[:, at[i]] = q_grad[i].astype(BF16)
                k_v[:, at[i]] = k_grad[i].astype(BF16)
                v_v[:, at[i]] = v_grad[i].astype(BF16)
        heads_of(some, c)

    cz, cx, cy = colors

    def up_down(color, pair, u):
        color.go(0, 2 * pair, u)
        color.go(0, 2 * pair + 1, u)

    def paced(color, pair, u):
        n = 4 * pair + u - 2
        for up in range(2):
            color.left(0, 2 * (n // 4) + up, n % 4)
        up_down(color, pair, u)

    for i in range(3):
        product(i, 2)
        up_down(colors[i], 0, 0)
        up_down(colors[i], 0, 1)
    for offset in (1, 3, 0):
        for i in range(3):
            product(i, offset)
    for item in ((1, 2), (1, 3), (2, 0), (2, 1)):
        scan2.step(*item)
    for color in colors:
        paced(color, 0, 2)
    for item in ((2, 2), (3, 0)):
        scan2.step(*item)
    for color in colors:
        paced(color, 0, 3)
    for item in ((2, 3), (3, 1)):
        scan2.step(*item)
    for u in range(4):
        up_down(cz, 1, u)
    paced(cx, 1, 0)
    paced(cy, 1, 0)
    for item in ((4, 0), (3, 2)):
        scan2.step(*item)
    cz.relay(0, 0)
    paced(cx, 1, 1)
    paced(cy, 1, 1)
    cz.relay(0, 1)
    cz.relay(0, 2)
    for item in ((4, 1), (3, 3)):
        scan2.step(*item)
    up_down(cx, 1, 2)
    up_down(cx, 1, 3)
    paced(cy, 1, 2)
    cz.relay(0, 3)
    for u in range(4):
        cx.relay(0, u)
    scan2.step(4, 2)
    paced(cy, 1, 3)
    scan2.step(4, 3)
    for u in range(4):
        cy.relay(0, u)

    def finish_first(color, u):
        color.finish(0, u)
        if u == 0:
            color.go(1, 0)
            color.go(1, 1)
        elif u == 1:
            color.go(1, 2)
        elif u == 2:
            color.go(1, 3)

    for u in range(4):
        scan2.step(5, u)
        backward_heads(u)
        finish_first(cz, u)
        finish_first(cx, u)
    for u in range(4):
        finish_first(cy, u)
    for color in colors:
        color.relay(1)
    for color in colors:
        color.finish(1)
        for kind in range(4):
            color.go(2, kind)
    for color in colors:
        color.relay(2)
    for i, color in enumerate(colors):
        color.finish(2, to=(wg_v, STARTS[i], WIDTHS[i]))

    for stage in range(1, 5):
        scan1.drain(stage)
    for stage in range(5):
        scan2.drain(stage)
    for color in colors:
        color.drain()
    for c in range(N_CHUNK):
        for copy in att_copies(c):
            copy.wait_send()


def store_kernel(*refs):
    sources, targets, sems = refs[:5], refs[5:10], refs[10]
    copies = [
        pltpu.make_async_copy(src, dst.at[0] if i < 4 else dst, sems.at[i])
        for i, (src, dst) in enumerate(zip(sources, targets))
    ]
    for copy in copies:
        copy.start()
    for copy in copies:
        copy.wait()


def body(queries, keys, values, out_grad, out_weight):
    vm = pltpu.VMEM
    dma = pltpu.SemaphoreType.DMA

    def scan_bufs():
        return [
            vm((4, 4, 128, 128), F32), vm((4, 4, 32, 128), F32), vm((4, 4, 32, 128), F32),
            vm((4, 32, 128), F32), vm((4, 4, 32, 128), F32), vm((4, 4, 32, 128), F32),
            vm((4, 4, 128, 128), F32),
        ]

    scratch = [
        vm((2 * TOK, D), BF16), vm((2, W_ROWS, D), BF16),
        vm((TOK, HD), F32), vm((TOK, HD), F32), vm((TOK, HD), BF16),
        vm((2, 4, 4, 4, 16, TOK), BF16), vm((4, 4, 4, 16, TOK), BF16),
        vm((8, 2, 4, 16, TOK), F32), vm((8, 2, 4, 16, TOK), F32),
        vm((4, 4, 128, 128), F32),
        *scan_bufs(), *scan_bufs(),
        *[vm((4, 4, 4, 2, 8, w), F32) for w in WIDTHS],
    ]
    scratch += [vm((6, 4, 4, 8, w), F32) for w in WIDTHS]
    scratch += [vm((6, 4, 8, w), F32) for w in WIDTHS]
    scratch += [vm((6, 8, w), F32) for w in WIDTHS]
    scratch += [
        dma((4,)), dma((2,)),
        dma((4, 5, 4)), dma((4, 5, 4)), dma((4, 5, 4)), dma((4, 5, 4)),
        dma((3, 36)), dma((3, 36)), dma((3,)), dma((3,)), dma((8,)), dma((8,)),
    ]
    any_space = pl.BlockSpec(memory_space=pl.ANY)
    in_vmem = pl.BlockSpec(memory_space=vm)
    results = pl.pallas_call(
        kernel,
        out_shape=(vm((TOK, HD), BF16),) * 4 + (vm((2, 8, D), F32),),
        in_specs=[any_space] * 5,
        out_specs=(in_vmem,) * 5,
        scratch_shapes=scratch,
        compiler_params=pltpu.CompilerParams(
            collective_id=0, has_side_effects=True, vmem_limit_bytes=VMEM_LIMIT
        ),
        name="block",
    )(queries, keys, values, out_grad, out_weight)
    flat = jax.ShapeDtypeStruct((1, TOK, HD), BF16)
    attended, d_query, d_key, d_value, weight_grad = pl.pallas_call(
        store_kernel,
        out_shape=(flat,) * 4 + (jax.ShapeDtypeStruct((2, 8, D), F32),),
        in_specs=[in_vmem] * 5,
        out_specs=(any_space,) * 5,
        scratch_shapes=[dma((5,))],
        compiler_params=pltpu.CompilerParams(vmem_limit_bytes=1 << 20),
        name="store",
    )(*results)
    return attended, d_query, d_key, d_value, weight_grad.reshape(16, D)


def solution(mesh):
    split = Mesh(mesh.devices.reshape(mesh.shape[DP], 4, 4, 4), DP_SEQ)
    rows = P(DP, SEQ, None)
    return jax.shard_map(
        body, mesh=split, in_specs=(rows, rows, rows, rows, P()),
        out_specs=(rows, rows, rows, rows, P(DP_SEQ, None)), check_vma=False,
    )
```

```python
import functools

import jax
import jax.numpy as jnp
from jax import lax
from jax.experimental import pallas as pl
from jax.experimental.pallas import tpu as pltpu
from jax.sharding import Mesh
from jax.sharding import PartitionSpec as P

P_SIZE = 128
H = 16
HD = 2048
D = 4096
TOK = 256
EPS = 1e-06
F32 = jnp.float32
BF16 = jnp.bfloat16
MESH = pl.DeviceIdType.MESH
DP = "dp"
SEQ = ("seq_0", "seq_1", "seq_2")
DP_SEQ = (DP,) + SEQ
N_CHUNK = 4
WIDTHS = (1536, 1408, 1152)
STARTS = (0, 1536, 2944)
ORDERS = ((0, 1, 2), (1, 2, 0), (2, 0, 1))
COL = 256
W_ROWS = 256
W_TILES = HD // W_ROWS
W_SLOTS = 3
VMEM_LIMIT = 62_500_000


def dot_nn(a, b):
    return lax.dot_general(a, b, (((1,), (0,)), ((), ())), preferred_element_type=F32)


def dot_nt(a, b):
    return lax.dot_general(a, b, (((1,), (1,)), ((), ())), preferred_element_type=F32)


def dot_tn(a, b):
    return lax.dot_general(a, b, (((0,), (0,)), ((), ())), preferred_element_type=F32)


def two_parts(x):
    high = x.astype(BF16)
    return high, (x - high.astype(F32)).astype(BF16)


def send(src, dst, send_sem, recv_sem, device):
    return pltpu.make_async_remote_copy(
        src_ref=src, dst_ref=dst, send_sem=send_sem, recv_sem=recv_sem,
        device_id=device, device_id_type=MESH,
    )


def scoped(f):
    @functools.wraps(f)
    def named(*args):
        with jax.named_scope(f.__name__ + "_" + "".join(map(str, args))):
            return f(*args)
    return named


class Scan:
    def __init__(self, where, bufs, sems, reverse):
        self.z, self.x, self.y = where
        self.S, self.YR, self.T, self.XR, self.PT, self.ZR, self.XC, self.R = bufs
        self.ss, self.rs = sems
        self.reverse = reverse

    def order(self):
        return range(3, -1, -1) if self.reverse else range(4)

    def copies(self, stage, c):
        out = []
        for r in range(1, 4):
            s, v = self.ss.at[stage], self.rs.at[c, stage]
            yt, xt, zt = (self.y + r) % 4, (self.x + r) % 4, (self.z + r) % 4
            if stage == 0:
                out.append(send(self.S.at[yt, c], self.YR.at[c, self.y], s, v, {SEQ[2]: yt}))
            elif stage == 1:
                out.append(send(self.T.at[c, xt], self.XR.at[c, self.x], s, v, {SEQ[1]: xt}))
            elif stage == 2:
                out.append(send(self.PT.at[c], self.ZR.at[c, self.z], s, v, {SEQ[0]: zt}))
            elif stage == 3:
                out.append(send(self.XR.at[c, xt], self.XC.at[c, self.x], s, v, {SEQ[1]: xt}))
            else:
                out.append(send(self.YR.at[c, yt], self.R.at[self.y, c], s, v, {SEQ[2]: yt}))
        return out

    def landing(self, stage, c):
        ref = (
            self.YR.at[c, 0:3], self.XR.at[c, 0:3], self.ZR.at[c, 0:3], self.XC.at[c, 0:3], self.R.at[0:3, c]
        )[stage]
        send(ref, ref, self.ss.at[stage], self.rs.at[c, stage], {SEQ[2]: (self.y + 1) % 4}).wait_recv()

    def go(self, stage, c):
        for copy in self.copies(stage, c):
            copy.start()

    def step(self, s, c):
        with jax.named_scope(f"scan{int(self.reverse)}_{s}{c}"):
            self.step_in(s, c)

    def step_in(self, s, c):
        if s > 0:
            self.landing(s - 1, c)
        if s == 0:
            self.YR[c, self.y] = self.S[self.y, c]
        elif s == 1:
            running = None
            for k in self.order():
                now = self.YR[c, k]
                self.YR[c, k] = jnp.zeros_like(now) if running is None else running
                running = now if running is None else running + now
            self.T[c] = running.reshape(4, 32, 128)
            self.XR[c, self.x] = self.T[c, self.x]
        elif s == 2:
            running = None
            for k in self.order():
                now = self.XR[c, k]
                self.XR[c, k] = jnp.zeros_like(now) if running is None else running
                running = now if running is None else running + now
            self.PT[c] = running
            self.ZR[c, self.z] = running
        elif s == 3:
            base = jnp.zeros((32, 128), F32)
            for k in range(4):
                passed = (self.z < k) if self.reverse else (self.z > k)
                base = base + jnp.where(passed, self.ZR[c, k], 0.0)
            for k in range(4):
                self.XR[c, k] = self.XR[c, k] + base
            self.XC[c, self.x] = self.XR[c, self.x]
        elif s == 4:
            carry = self.XC[c].reshape(128, 128)
            for k in range(4):
                self.YR[c, k] = self.YR[c, k] + carry
            self.R[self.y, c] = self.YR[c, self.y]
        if s < 5:
            self.go(s, c)

    def drain(self, stage):
        ref = (self.S.at[0:3], self.T.at[:, 0:3], self.T.at[:, 0:3], self.T.at[:, 0:3], self.S.at[0:3])[stage]
        send(ref, ref, self.ss.at[stage], self.rs.at[0, stage], {SEQ[2]: (self.y + 1) % 4}).wait_send()


class Color:
    def __init__(self, where, order, part, recv, ss, rs):
        self.where, self.order, self.part, self.recv, self.ss, self.rs = where, order, part, recv, ss, rs
        self.gone = set()

    def axis(self, phase):
        return self.order[phase]

    def slot(self, phase, t, u):
        idx = [slice(None)] * 3
        for p in range(phase):
            idx[self.order[p]] = self.where[self.order[p]]
        idx[self.order[phase]] = t
        if phase < 2:
            nxt = self.order[phase + 1]
            idx[nxt] = (self.where[nxt] + (2, 1, 3, 0)[u]) % 4
        return idx

    def sems(self, phase, kind, u):
        leave = 4 * (kind // 2) + u if phase == 0 else 11 + phase
        land = 8 * phase + 2 * u + (0 if kind < 2 else 1)
        return self.ss.at[leave], self.rs.at[land]

    def copy(self, phase, kind, u=0):
        a = self.axis(phase)
        m = self.where[a]
        up = kind % 2 == 0
        to = (m + 1) % 4 if up else (m + 3) % 4
        t = (m + 2) % 4 if kind < 2 else to
        half = (0, 1, 1, 0, 0, 1)[kind]
        src = self.part.at[tuple(self.slot(phase, t, u)) + (half,)]
        dst = self.recv[phase].at[kind, u] if phase < 2 else self.recv[phase].at[kind]
        return send(src, dst, *self.sems(phase, kind, u), {SEQ[a]: to})

    def go(self, phase, kind, u=0):
        self.copy(phase, kind, u).start()

    def bulk(self, phase, kinds, u, ref):
        a = self.axis(phase)
        return send(ref, ref, *self.sems(phase, kinds.start, u), {SEQ[a]: (self.where[a] + 1) % 4})

    def left(self, pair, u):
        if (pair, u) not in self.gone:
            self.gone.add((pair, u))
            kinds = slice(2 * pair, 2 * pair + 2)
            self.bulk(0, kinds, u, self.recv[0].at[kinds, u]).wait_send()

    def landed(self, phase, kinds, u):
        ref = self.recv[phase].at[kinds, u] if phase < 2 else self.recv[phase].at[kinds]
        self.bulk(phase, kinds, u, ref).wait_recv()

    def got(self, phase, kind, u=0):
        return self.recv[phase][kind, u] if phase < 2 else self.recv[phase][kind]

    def relay(self, phase, u=0):
        with jax.named_scope(f"relay{self.order[0]}_{phase}{u}"):
            self.relay_in(phase, u)

    def relay_in(self, phase, u=0):
        m = self.where[self.axis(phase)]
        self.landed(phase, slice(0, 2), u)
        for kind, to, half in ((0, (m + 1) % 4, 0), (1, (m + 3) % 4, 1)):
            more = self.got(phase, kind, u)
            at = tuple(self.slot(phase, to, u)) + (half,)
            self.part[at] = self.part[at] + more
            self.go(phase, 4 + kind, u)

    def finish(self, phase, u=0, to=None):
        with jax.named_scope(f"finish{self.order[0]}_{phase}{u}"):
            self.finish_in(phase, u, to)

    def finish_in(self, phase, u=0, to=None):
        m = self.where[self.axis(phase)]
        self.landed(phase, slice(2, 6), u)
        for half, kinds in ((0, (3, 4)), (1, (2, 5))):
            more = self.got(phase, kinds[0], u) + self.got(phase, kinds[1], u)
            at = tuple(self.slot(phase, m, u)) + (half,)
            if to is None:
                self.part[at] = self.part[at] + more
            else:
                out, start, width = to
                out[half, :, start:start + width] = self.part[at] + more

    def drain(self, phase):
        if phase == 0:
            for pair in range(3):
                for u in range(4):
                    self.left(pair, u)
        else:
            self.bulk(phase, slice(0, 6), 0, self.recv[phase]).wait_send()


def kernel(
    q_hbm, k_hbm, v_hbm, og_hbm, w_hbm,
    att_v, q_v, k_v, v_v, wg_v,
    og_v, w_v, grad_v, intra_v, do_v, attT, attP, attS, attR,
    state, yr1, t1, xr1, pt1, zr1, xc1, r1,
    yr2, t2, xr2, pt2, zr2, xc2, r2,
    p0, p1, p2, a0, a1, a2, b0, b1, b2, c0, c1, c2,
    in_sem, w_sem, s1s, s1r, s2s, s2r, css, crs, ogs, ogr, ats, atr,
):
    d = lax.axis_index(DP)
    where = tuple(lax.axis_index(a) for a in SEQ)
    z, x, y = where
    other = {DP: 1 - d}
    parts = (p0, p1, p2)

    loads = [
        pltpu.make_async_copy(src.at[0], dst, in_sem.at[i])
        for i, (src, dst) in enumerate(((k_hbm, k_v), (v_hbm, v_v), (og_hbm, og_v.at[:TOK]), (q_hbm, q_v)))
    ]
    for load in loads:
        load.start()

    def w_load(i):
        return pltpu.make_async_copy(
            w_hbm.at[pl.ds(pl.multiple_of(i * W_ROWS, W_ROWS), W_ROWS)], w_v.at[i % W_SLOTS], w_sem.at[i % W_SLOTS]
        )

    for i in range(W_SLOTS):
        w_load(i).start()

    barrier = pltpu.get_barrier_semaphore()
    pl.semaphore_signal(barrier, inc=1, device_id=other, device_id_type=MESH)
    for a in range(3):
        for r in range(1, 4):
            pl.semaphore_signal(barrier, inc=1, device_id={SEQ[a]: (where[a] + r) % 4}, device_id_type=MESH)

    scan1 = Scan(where, (state, yr1, t1, xr1, pt1, zr1, xc1, r1), (s1s, s1r), False)
    scan2 = Scan(where, (state, yr2, t2, xr2, pt2, zr2, xc2, r2), (s2s, s2r), True)
    colors = [
        Color(where, ORDERS[i], parts[i], ((a0, b0, c0), (a1, b1, c1), (a2, b2, c2))[i], css.at[i], crs.at[i])
        for i in range(3)
    ]

    def cols(h):
        return pl.ds(pl.multiple_of(h * P_SIZE, P_SIZE), P_SIZE)

    def heads_of(fn, c, width=2):
        def one(n, carry):
            fn([n * width + i for i in range(width)], c)
            return carry
        lax.fori_loop(0, 4 // width, one, 0)

    @scoped
    def states(c):
        def some(js, c):
            at = [cols(4 * j + c) for j in js]
            out = [dot_tn(k_v[:, a], v_v[:, a]) for a in at]
            for j, value in zip(js, out):
                state[j, c] = value
        heads_of(some, c)

    with jax.named_scope("load"):
        loads[0].wait()
        loads[1].wait()
    states(0)
    with jax.named_scope("enter"):
        pl.semaphore_wait(barrier, 10)
    scan1.step(0, 0)
    for c in range(1, N_CHUNK):
        states(c)
        scan1.step(0, c)

    loads[2].wait()

    def og_copy(i):
        return send(parts[i].at[0], parts[i].at[1], ogs.at[i], ogr.at[i], other)

    for i in range(3):
        def put(n, carry, i=i):
            rows = pl.ds(pl.multiple_of(n * 64, 64), 64)
            block = og_v[rows, STARTS[i]:STARTS[i] + WIDTHS[i]].astype(F32)
            parts[i][0, n] = block.reshape(4, 2, 8, WIDTHS[i])
            return carry
        lax.fori_loop(0, 4, put, 0)
        og_copy(i).start()

    @scoped
    def grad_tiles(lo, hi):
        def one(i, carry):
            w_load(i).wait()
            block = dot_nt(og_v[:TOK], w_v[i % W_SLOTS])
            at = pl.ds(pl.multiple_of(i * W_ROWS, W_ROWS), W_ROWS)
            grad_v[:, at] = block

            @pl.when(i + W_SLOTS < W_TILES)
            def _():
                w_load(i + W_SLOTS).start()
            return carry
        lax.fori_loop(lo, hi, one, 0)

    @scoped
    def og_take(i):
        og_copy(i).wait_recv()
        def take(n, carry):
            rows = pl.ds(pl.multiple_of(TOK + n * 64, 64), 64)
            block = parts[i][1, n].reshape(64, WIDTHS[i])
            og_v[rows, STARTS[i]:STARTS[i] + WIDTHS[i]] = block.astype(BF16)
            return carry
        lax.fori_loop(0, 4, take, 0)

    lower = (
        lax.broadcasted_iota(jnp.int32, (TOK, TOK), 0) >= lax.broadcasted_iota(jnp.int32, (TOK, TOK), 1)
    )

    @scoped
    def inside_heads(c):
        def some(js, c):
            at = [cols(4 * j + c) for j in js]
            scores = [dot_nt(q_v[:, a], k_v[:, a]) for a in at]
            probs = [jnp.where(lower, x, 0.0).astype(BF16) for x in scores]
            out = [dot_nn(p, v_v[:, a]) for p, a in zip(probs, at)]
            for a, value in zip(at, out):
                intra_v[:, a] = value
        heads_of(some, c)

    @scoped
    def forward_heads(c):
        def some(js, c):
            at = [cols(4 * j + c) for j in js]
            q = [q_v[:, a] for a in at]
            split = [two_parts(r1[j, c]) for j in js]
            inter = [dot_nn(a, high) + dot_nn(a, low) for a, (high, low) in zip(q, split)]
            o = [intra_v[:, a] + x for a, x in zip(at, inter)]
            inverse = [lax.rsqrt(jnp.mean(x * x, axis=-1, keepdims=True) + EPS) for x in o]
            normed = [x * i for x, i in zip(o, inverse)]
            grad = [grad_v[:, a] for a in at]
            level = [jnp.mean(g * n, axis=-1, keepdims=True) for g, n in zip(grad, normed)]
            d_o = [(i * (g - n * m)).astype(BF16) for i, g, n, m in zip(inverse, grad, normed, level)]
            d_prefix = [dot_tn(a, b) for a, b in zip(q, d_o)]
            att = [n.astype(BF16) for n in normed]
            turned = [a.astype(F32).T.astype(BF16).reshape(2, 4, 16, TOK) for a in att]
            for i, j in enumerate(js):
                h = 4 * j + c
                hh = h % 8
                att_v[:, at[i]] = att[i]
                do_v[:, at[i]] = d_o[i]
                state[j, c] = d_prefix[i]
                attT[h // 8, hh // 2, pl.ds(2 * (hh % 2), 2)] = turned[i]
        heads_of(some, c)

    def att_copies(c):
        return [
            send(attS.at[2 * c + i], attR.at[2 * c + i], ats.at[0], atr.at[c], other)
            for i in range(2)
        ]

    @scoped
    def att_give(c):
        for i, copy in enumerate(att_copies(c)):
            hh = 4 * i + c
            attS[2 * c + i] = attT[1 - d, hh // 2, 2 * (hh % 2):2 * (hh % 2) + 2].astype(F32)
            copy.start()

    @scoped
    def att_take(c):
        both = attR.at[2 * c:2 * c + 2]
        send(both, both, ats.at[0], atr.at[c], other).wait_recv()
        for i in range(2):
            hh = 4 * i + c
            attP[hh // 2, 2 * (hh % 2):2 * (hh % 2) + 2] = attR[2 * c + i].astype(BF16)

    forward = (
        (grad_tiles, 0, 4), (1, 0), (grad_tiles, 4, 6), (1, 1), (grad_tiles, 6, 8), (2, 0), (1, 2),
        (inside_heads, 0), (2, 1), (1, 3), (inside_heads, 1), (3, 0), (2, 2), (og_take, 0), (inside_heads, 2),
        (3, 1), (2, 3), (4, 0), (inside_heads, 3), (3, 2), (4, 1), (3, 3), (og_take, 1), (4, 2), (og_take, 2),
        (4, 3),
    )
    loads[3].wait()
    for item in forward:
        if callable(item[0]):
            item[0](*item[1:])
        else:
            scan1.step(*item)
    scan1.drain(0)
    for c in range(N_CHUNK):
        scan1.step(5, c)
        forward_heads(c)
        scan2.step(0, c)
        att_give(c)
    for c in range(N_CHUNK):
        att_take(c)
    for i in range(3):
        og_copy(i).wait_send()

    @scoped
    def product(i, offset):
        color = colors[i]
        axis = ORDERS[i][0]
        t = (where[axis] + offset) % 4
        idx = [slice(None)] * 3
        idx[axis] = t
        idx = tuple(idx)
        both = jnp.concatenate([attT[(d,) + idx].reshape(TOK, TOK), attP[idx].reshape(TOK, TOK)], axis=1)
        for low in range(0, WIDTHS[i], COL):
            high = min(low + COL, WIDTHS[i])
            block = dot_nn(both, og_v[:, STARTS[i] + low:STARTS[i] + high])
            color.part[idx + (slice(None), slice(None), slice(low, high))] = block.reshape(4, 4, 2, 8, high - low)

    @scoped
    def backward_heads(c):
        def some(js, c):
            at = [cols(4 * j + c) for j in js]
            q, k, v, d_o = ([ref[:, a] for a in at] for ref in (q_v, k_v, v_v, do_v))
            probs = [jnp.where(lower, dot_nt(a, b), 0.0).astype(BF16) for a, b in zip(q, k)]
            d_probs = [jnp.where(lower, dot_nt(a, b), 0.0).astype(BF16) for a, b in zip(d_o, v)]
            before = [two_parts(r1[j, c]) for j in js]
            after = [two_parts(r2[j, c]) for j in js]
            n = range(len(js))
            q_grad = [dot_nn(d_probs[i], k[i]) + sum(dot_nt(d_o[i], p) for p in before[i]) for i in n]
            k_grad = [dot_tn(d_probs[i], q[i]) + sum(dot_nt(v[i], p) for p in after[i]) for i in n]
            v_grad = [dot_tn(probs[i], d_o[i]) + sum(dot_nn(k[i], p) for p in after[i]) for i in n]
            for i in n:
                q_v[:, at[i]] = q_grad[i].astype(BF16)
                k_v[:, at[i]] = k_grad[i].astype(BF16)
                v_v[:, at[i]] = v_grad[i].astype(BF16)
        heads_of(some, c)

    cz, cx, cy = colors

    def up_down(color, pair, u):
        color.go(0, 2 * pair, u)
        color.go(0, 2 * pair + 1, u)

    def paced(color, pair, u):
        n = 4 * pair + u - 2
        color.left(n // 4, n % 4)
        up_down(color, pair, u)

    for i in range(3):
        product(i, 2)
        up_down(colors[i], 0, 0)
        up_down(colors[i], 0, 1)
    up_down(cz, 0, 2)
    scan2.step(1, 0)
    for i in range(3):
        product(i, 1)
    scan2.step(1, 1)
    for offset in (3, 0):
        for i in range(3):
            product(i, offset)
    paced(cx, 0, 2)
    paced(cy, 0, 2)
    for item in ((1, 2), (1, 3), (2, 0), (2, 1)):
        scan2.step(*item)
    for stage in range(1, 5):
        scan1.drain(stage)
    for color in colors:
        paced(color, 0, 3)
    for item in ((2, 2), (3, 0)):
        scan2.step(*item)
    paced(cx, 1, 0)
    paced(cy, 1, 0)
    for item in ((2, 3), (3, 1)):
        scan2.step(*item)
    for u in range(4):
        up_down(cz, 1, u)
    paced(cx, 1, 1)
    scan2.step(4, 0)
    scan2.step(3, 2)
    paced(cx, 1, 2)
    paced(cy, 1, 1)
    cz.relay(0, 0)
    cz.relay(0, 1)
    scan2.step(4, 1)
    scan2.step(3, 3)
    up_down(cx, 1, 3)
    cz.relay(0, 2)
    cz.relay(0, 3)
    for u in range(4):
        cx.relay(0, u)
    paced(cy, 1, 2)
    scan2.step(4, 2)
    paced(cy, 1, 3)
    scan2.step(4, 3)
    for u in range(4):
        cy.relay(0, u)

    def finish_first(color, u):
        color.finish(0, u)
        for v in range(4):
            if u == 0:
                color.go(1, 0, v)
                color.go(1, 1, v)
            elif u < 3:
                color.go(1, 1 + u, v)

    def finish_second(color, v):
        color.finish(1, v)
        if v == 0:
            color.go(2, 0)
            color.go(2, 1)
        elif v < 3:
            color.go(2, 1 + v)

    for u in range(3):
        scan2.step(5, u)
        backward_heads(u)
    finish_first(cx, 0)
    scan2.step(5, 3)
    backward_heads(3)
    for color, u in (
        (cz, 0), (cx, 1), (cy, 0), (cz, 1), (cx, 2), (cy, 1), (cx, 3), (cz, 2), (cy, 2), (cz, 3), (cy, 3)
    ):
        finish_first(color, u)
    for stage in range(5):
        scan2.drain(stage)
    send(attS, attS, ats.at[0], atr.at[0], other).wait_send()
    for color in colors:
        color.drain(0)
    for v in range(4):
        for color in (cx, cz, cy):
            color.relay(1, v)
    for v in range(4):
        for color in (cx, cz, cy):
            finish_second(color, v)
    for color in colors:
        color.drain(1)
    for color in (cx, cz, cy):
        color.relay(2)
    for i in (1, 0, 2):
        colors[i].finish(2, to=(wg_v, STARTS[i], WIDTHS[i]))
    for color in colors:
        color.drain(2)


def store_kernel(*refs):
    sources, targets, sems = refs[:5], refs[5:10], refs[10]
    copies = [
        pltpu.make_async_copy(src, dst.at[0] if i < 4 else dst, sems.at[i])
        for i, (src, dst) in enumerate(zip(sources, targets))
    ]
    for copy in copies:
        copy.start()
    for copy in copies:
        copy.wait()


def body(queries, keys, values, out_grad, out_weight):
    vm = pltpu.VMEM
    dma = pltpu.SemaphoreType.DMA

    def scan_bufs():
        return [
            vm((4, 4, 128, 128), F32), vm((4, 4, 32, 128), F32), vm((4, 4, 32, 128), F32),
            vm((4, 32, 128), F32), vm((4, 4, 32, 128), F32), vm((4, 4, 32, 128), F32),
            vm((4, 4, 128, 128), F32),
        ]

    scratch = [
        vm((2 * TOK, D), BF16), vm((W_SLOTS, W_ROWS, D), BF16),
        vm((TOK, HD), F32), vm((TOK, HD), F32), vm((TOK, HD), BF16),
        vm((2, 4, 4, 4, 16, TOK), BF16), vm((4, 4, 4, 16, TOK), BF16),
        vm((8, 2, 4, 16, TOK), F32), vm((8, 2, 4, 16, TOK), F32),
        vm((4, 4, 128, 128), F32),
        *scan_bufs(), *scan_bufs(),
        *[vm((4, 4, 4, 2, 8, w), F32) for w in WIDTHS],
    ]
    scratch += [vm((6, 4, 4, 8, w), F32) for w in WIDTHS]
    scratch += [vm((6, 4, 8, w), F32) for w in WIDTHS]
    scratch += [vm((6, 8, w), F32) for w in WIDTHS]
    scratch += [
        dma((4,)), dma((W_SLOTS,)),
        dma((5,)), dma((4, 5)), dma((5,)), dma((4, 5)),
        dma((3, 14)), dma((3, 18)), dma((3,)), dma((3,)), dma((1,)), dma((4,)),
    ]
    any_space = pl.BlockSpec(memory_space=pl.ANY)
    in_vmem = pl.BlockSpec(memory_space=vm)
    results = pl.pallas_call(
        kernel,
        out_shape=(vm((TOK, HD), BF16),) * 4 + (vm((2, 8, D), F32),),
        in_specs=[any_space] * 5,
        out_specs=(in_vmem,) * 5,
        scratch_shapes=scratch,
        compiler_params=pltpu.CompilerParams(
            collective_id=0, has_side_effects=True, vmem_limit_bytes=VMEM_LIMIT
        ),
        name="block",
    )(queries, keys, values, out_grad, out_weight)
    flat = jax.ShapeDtypeStruct((1, TOK, HD), BF16)
    attended, d_query, d_key, d_value, weight_grad = pl.pallas_call(
        store_kernel,
        out_shape=(flat,) * 4 + (jax.ShapeDtypeStruct((2, 8, D), F32),),
        in_specs=[in_vmem] * 5,
        out_specs=(any_space,) * 5,
        scratch_shapes=[dma((5,))],
        compiler_params=pltpu.CompilerParams(vmem_limit_bytes=1 << 20),
        name="store",
    )(*results)
    return attended, d_query, d_key, d_value, weight_grad.reshape(16, D)


def solution(mesh):
    split = Mesh(mesh.devices.reshape(mesh.shape[DP], 4, 4, 4), DP_SEQ)
    rows = P(DP, SEQ, None)
    return jax.shard_map(
        body, mesh=split, in_specs=(rows, rows, rows, rows, P()),
        out_specs=(rows, rows, rows, rows, P(DP_SEQ, None)), check_vma=False,
    )
```

```python
import functools

import jax
import jax.numpy as jnp
from jax import lax
from jax.experimental import pallas as pl
from jax.experimental.pallas import tpu as pltpu
from jax.sharding import Mesh
from jax.sharding import PartitionSpec as P

P_SIZE = 128
H = 16
HD = 2048
D = 4096
TOK = 256
EPS = 1e-06
F32 = jnp.float32
BF16 = jnp.bfloat16
MESH = pl.DeviceIdType.MESH
DP = "dp"
SEQ = ("seq_0", "seq_1", "seq_2")
DP_SEQ = (DP,) + SEQ
N_CHUNK = 4
WIDTHS = (1536, 1408, 1152)
STARTS = (0, 1536, 2944)
ORDERS = ((0, 1, 2), (1, 2, 0), (2, 0, 1))
COL = 256
W_ROWS = 256
W_TILES = HD // W_ROWS
W_SLOTS = 3
VMEM_LIMIT = 62_500_000


def dot_nn(a, b):
    return lax.dot_general(a, b, (((1,), (0,)), ((), ())), preferred_element_type=F32)


def dot_nt(a, b):
    return lax.dot_general(a, b, (((1,), (1,)), ((), ())), preferred_element_type=F32)


def dot_tn(a, b):
    return lax.dot_general(a, b, (((0,), (0,)), ((), ())), preferred_element_type=F32)


def two_parts(x):
    high = x.astype(BF16)
    return high, (x - high.astype(F32)).astype(BF16)


def send(src, dst, send_sem, recv_sem, device):
    return pltpu.make_async_remote_copy(
        src_ref=src, dst_ref=dst, send_sem=send_sem, recv_sem=recv_sem,
        device_id=device, device_id_type=MESH,
    )


def scoped(f):
    @functools.wraps(f)
    def named(*args):
        with jax.named_scope(f.__name__ + "_" + "".join(str(a) for a in args if isinstance(a, int))):
            return f(*args)
    return named


class Scan:
    def __init__(self, where, bufs, sems, reverse):
        self.z, self.x, self.y = where
        self.S, self.YR, self.T, self.XR, self.PT, self.ZR, self.XC, self.R = bufs
        self.ss, self.rs = sems
        self.reverse = reverse

    def order(self):
        return range(3, -1, -1) if self.reverse else range(4)

    def copies(self, stage, c):
        out = []
        for r in (2, 1, 3):
            s, v = self.ss.at[stage], self.rs.at[c, stage]
            yt, xt, zt = (self.y + r) % 4, (self.x + r) % 4, (self.z + r) % 4
            if stage == 0:
                out.append(send(self.S.at[yt, c], self.YR.at[c, self.y], s, v, {SEQ[2]: yt}))
            elif stage == 1:
                out.append(send(self.T.at[c, xt], self.XR.at[c, self.x], s, v, {SEQ[1]: xt}))
            elif stage == 2:
                out.append(send(self.PT.at[c], self.ZR.at[c, self.z], s, v, {SEQ[0]: zt}))
            elif stage == 3:
                out.append(send(self.XR.at[c, xt], self.XC.at[c, self.x], s, v, {SEQ[1]: xt}))
            else:
                out.append(send(self.YR.at[c, yt], self.R.at[self.y, c], s, v, {SEQ[2]: yt}))
        return out

    def landing(self, stage, c):
        ref = (
            self.YR.at[c, 0:3], self.XR.at[c, 0:3], self.ZR.at[c, 0:3], self.XC.at[c, 0:3], self.R.at[0:3, c]
        )[stage]
        send(ref, ref, self.ss.at[stage], self.rs.at[c, stage], {SEQ[2]: (self.y + 1) % 4}).wait_recv()

    def go(self, stage, c):
        for copy in self.copies(stage, c):
            copy.start()

    def step(self, s, c):
        with jax.named_scope(f"scan{int(self.reverse)}_{s}{c}"):
            self.step_in(s, c)

    def step_in(self, s, c):
        if s > 0:
            self.landing(s - 1, c)
        if s == 0:
            self.YR[c, self.y] = self.S[self.y, c]
        elif s == 1:
            running = None
            for k in self.order():
                now = self.YR[c, k]
                self.YR[c, k] = jnp.zeros_like(now) if running is None else running
                running = now if running is None else running + now
            self.T[c] = running.reshape(4, 32, 128)
            self.XR[c, self.x] = self.T[c, self.x]
        elif s == 2:
            running = None
            for k in self.order():
                now = self.XR[c, k]
                self.XR[c, k] = jnp.zeros_like(now) if running is None else running
                running = now if running is None else running + now
            self.PT[c] = running
            self.ZR[c, self.z] = running
        elif s == 3:
            base = jnp.zeros((32, 128), F32)
            for k in range(4):
                passed = (self.z < k) if self.reverse else (self.z > k)
                base = base + jnp.where(passed, self.ZR[c, k], 0.0)
            for k in range(4):
                self.XR[c, k] = self.XR[c, k] + base
            self.XC[c, self.x] = self.XR[c, self.x]
        elif s == 4:
            carry = self.XC[c].reshape(128, 128)
            for k in range(4):
                self.YR[c, k] = self.YR[c, k] + carry
            self.R[self.y, c] = self.YR[c, self.y]
        if s < 5:
            self.go(s, c)

    def drain(self, stage):
        ref = (self.S.at[0:3], self.T.at[:, 0:3], self.T.at[:, 0:3], self.T.at[:, 0:3], self.S.at[0:3])[stage]
        send(ref, ref, self.ss.at[stage], self.rs.at[0, stage], {SEQ[2]: (self.y + 1) % 4}).wait_send()


class Color:
    def __init__(self, where, order, part, recv, ss, rs):
        self.where, self.order, self.part, self.recv, self.ss, self.rs = where, order, part, recv, ss, rs
        self.gone = set()

    def axis(self, phase):
        return self.order[phase]

    def slot(self, phase, t, u):
        idx = [slice(None)] * 3
        for p in range(phase):
            idx[self.order[p]] = self.where[self.order[p]]
        idx[self.order[phase]] = t
        if phase < 2:
            nxt = self.order[phase + 1]
            idx[nxt] = (self.where[nxt] + (2, 1, 3, 0)[u]) % 4
        return idx

    def sems(self, phase, kind, u):
        leave = 4 * (kind // 2) + u if phase == 0 else 11 + phase
        land = 8 * phase + 2 * u + (0 if kind < 2 else 1)
        return self.ss.at[leave], self.rs.at[land]

    def copy(self, phase, kind, u=0):
        a = self.axis(phase)
        m = self.where[a]
        up = kind % 2 == 0
        to = (m + 1) % 4 if up else (m + 3) % 4
        t = (m + 2) % 4 if kind < 2 else to
        half = (0, 1, 1, 0, 0, 1)[kind]
        src = self.part.at[tuple(self.slot(phase, t, u)) + (half,)]
        dst = self.recv[phase].at[kind, u]
        return send(src, dst, *self.sems(phase, kind, u), {SEQ[a]: to})

    def go(self, phase, kind, u=0):
        self.copy(phase, kind, u).start()

    def bulk(self, phase, kinds, u, ref):
        a = self.axis(phase)
        return send(ref, ref, *self.sems(phase, kinds.start, u), {SEQ[a]: (self.where[a] + 1) % 4})

    def left(self, pair, u):
        if (pair, u) not in self.gone:
            self.gone.add((pair, u))
            kinds = slice(2 * pair, 2 * pair + 2)
            self.bulk(0, kinds, u, self.recv[0].at[kinds, u]).wait_send()

    def landed(self, phase, kinds, u):
        self.bulk(phase, kinds, u, self.recv[phase].at[kinds, u]).wait_recv()

    def got(self, phase, kind, u=0):
        return self.recv[phase][kind, u]

    def relay(self, phase, u=0):
        with jax.named_scope(f"relay{self.order[0]}_{phase}{u}"):
            self.relay_in(phase, u)

    def relay_in(self, phase, u=0):
        m = self.where[self.axis(phase)]
        self.landed(phase, slice(0, 2), u)
        for kind, to, half in ((0, (m + 1) % 4, 0), (1, (m + 3) % 4, 1)):
            more = self.got(phase, kind, u)
            at = tuple(self.slot(phase, to, u)) + (half,)
            self.part[at] = self.part[at] + more
            self.go(phase, 4 + kind, u)

    def finish(self, phase, u=0):
        with jax.named_scope(f"finish{self.order[0]}_{phase}{u}"):
            self.finish_in(phase, u)

    def finish_in(self, phase, u=0):
        m = self.where[self.axis(phase)]
        self.landed(phase, slice(2, 6), u)
        for half, kinds in ((0, (3, 4)), (1, (2, 5))):
            more = self.got(phase, kinds[0], u) + self.got(phase, kinds[1], u)
            at = tuple(self.slot(phase, m, u)) + (half,)
            self.part[at] = self.part[at] + more

    def direct(self, r):
        a = self.axis(2)
        to = (self.where[a] + r) % 4
        src = self.part.at[tuple(self.slot(2, to, 0))]
        return send(src, self.recv[2].at[r - 1], *self.sems(2, 0, 0), {SEQ[a]: to})

    def last(self, out, start, width):
        with jax.named_scope(f"last{self.order[0]}"):
            self.bulk(2, slice(0, 6), 0, self.recv[2]).wait_recv()
            own = self.part[tuple(self.slot(2, self.where[self.axis(2)], 0))]
            total = (own + self.recv[2][0]) + (self.recv[2][1] + self.recv[2][2])
            out[:, :, start:start + width] = total

    def drain(self, phase):
        if phase == 0:
            for pair in range(3):
                for u in range(4):
                    self.left(pair, u)
        else:
            self.bulk(phase, slice(0, 6), 0, self.recv[phase]).wait_send()


def kernel(
    q_hbm, k_hbm, v_hbm, og_hbm, w_hbm,
    att_v, q_v, k_v, v_v, wg_v,
    og_v, w_v, grad_v, intra_v, do_v, attT, attP, attS, attR,
    state, yr1, t1, xr1, pt1, zr1, xc1, r1,
    yr2, t2, xr2, pt2, zr2, xc2, r2,
    p0, p1, p2, a0, a1, a2, b0, b1, b2, c0, c1, c2,
    in_sem, w_sem, s1s, s1r, s2s, s2r, css, crs, ogs, ogr, ats, atr,
):
    d = lax.axis_index(DP)
    where = tuple(lax.axis_index(a) for a in SEQ)
    z, x, y = where
    other = {DP: 1 - d}
    parts = (p0, p1, p2)

    loads = [
        pltpu.make_async_copy(src.at[0], dst, in_sem.at[i])
        for i, (src, dst) in enumerate(((k_hbm, k_v), (v_hbm, v_v), (og_hbm, og_v.at[:TOK]), (q_hbm, q_v)))
    ]
    loads[0].start()
    loads[1].start()

    def w_load(i):
        return pltpu.make_async_copy(
            w_hbm.at[pl.ds(pl.multiple_of(i * W_ROWS, W_ROWS), W_ROWS)], w_v.at[i % W_SLOTS], w_sem.at[i % W_SLOTS]
        )

    barrier = pltpu.get_barrier_semaphore()
    pl.semaphore_signal(barrier, inc=1, device_id=other, device_id_type=MESH)
    for a in range(3):
        for r in range(1, 4):
            pl.semaphore_signal(barrier, inc=1, device_id={SEQ[a]: (where[a] + r) % 4}, device_id_type=MESH)

    scan1 = Scan(where, (state, yr1, t1, xr1, pt1, zr1, xc1, r1), (s1s, s1r), False)
    scan2 = Scan(where, (state, yr2, t2, xr2, pt2, zr2, xc2, r2), (s2s, s2r), True)
    colors = [
        Color(where, ORDERS[i], parts[i], ((a0, b0, c0), (a1, b1, c1), (a2, b2, c2))[i], css.at[i], crs.at[i])
        for i in range(3)
    ]

    def cols(h):
        return pl.ds(pl.multiple_of(h * P_SIZE, P_SIZE), P_SIZE)

    def heads_of(fn, c, width=2):
        def one(n, carry):
            fn([n * width + i for i in range(width)], c)
            return carry
        lax.fori_loop(0, 4 // width, one, 0)

    @scoped
    def states(c):
        def some(js, c):
            at = [cols(4 * j + c) for j in js]
            out = [dot_tn(k_v[:, a], v_v[:, a]) for a in at]
            for j, value in zip(js, out):
                state[j, c] = value
        heads_of(some, c)

    with jax.named_scope("load"):
        loads[0].wait()
        loads[1].wait()
    loads[2].start()
    for i in range(W_SLOTS):
        w_load(i).start()
    loads[3].start()
    states(0)
    with jax.named_scope("enter"):
        pl.semaphore_wait(barrier, 10)
    scan1.step(0, 0)
    for c in range(1, N_CHUNK):
        states(c)
        scan1.step(0, c)

    loads[2].wait()

    def og_copy(i):
        return send(parts[i].at[0], parts[i].at[1], ogs.at[i], ogr.at[i], other)

    for i in range(3):
        def put(n, carry, i=i):
            rows = pl.ds(pl.multiple_of(n * 64, 64), 64)
            block = og_v[rows, STARTS[i]:STARTS[i] + WIDTHS[i]].astype(F32)
            parts[i][0, n] = block.reshape(4, 2, 8, WIDTHS[i])
            return carry
        lax.fori_loop(0, 4, put, 0)
        og_copy(i).start()

    @scoped
    def grad_tiles(lo, hi):
        def one(i, carry):
            w_load(i).wait()
            block = dot_nt(og_v[:TOK], w_v[i % W_SLOTS])
            at = pl.ds(pl.multiple_of(i * W_ROWS, W_ROWS), W_ROWS)
            grad_v[:, at] = block

            @pl.when(i + W_SLOTS < W_TILES)
            def _():
                w_load(i + W_SLOTS).start()
            return carry
        lax.fori_loop(lo, hi, one, 0)

    @scoped
    def og_take(i):
        og_copy(i).wait_recv()
        def take(n, carry):
            rows = pl.ds(pl.multiple_of(TOK + n * 64, 64), 64)
            block = parts[i][1, n].reshape(64, WIDTHS[i])
            og_v[rows, STARTS[i]:STARTS[i] + WIDTHS[i]] = block.astype(BF16)
            return carry
        lax.fori_loop(0, 4, take, 0)

    lower = (
        lax.broadcasted_iota(jnp.int32, (TOK, TOK), 0) >= lax.broadcasted_iota(jnp.int32, (TOK, TOK), 1)
    )

    @scoped
    def inside_heads(c):
        def some(js, c):
            at = [cols(4 * j + c) for j in js]
            scores = [dot_nt(q_v[:, a], k_v[:, a]) for a in at]
            probs = [jnp.where(lower, x, 0.0).astype(BF16) for x in scores]
            out = [dot_nn(p, v_v[:, a]) for p, a in zip(probs, at)]
            for a, value in zip(at, out):
                intra_v[:, a] = value
        heads_of(some, c)

    @scoped
    def forward_heads(c):
        def some(js, c):
            at = [cols(4 * j + c) for j in js]
            q = [q_v[:, a] for a in at]
            split = [two_parts(r1[j, c]) for j in js]
            inter = [dot_nn(a, high) + dot_nn(a, low) for a, (high, low) in zip(q, split)]
            o = [intra_v[:, a] + x for a, x in zip(at, inter)]
            inverse = [lax.rsqrt(jnp.mean(x * x, axis=-1, keepdims=True) + EPS) for x in o]
            normed = [x * i for x, i in zip(o, inverse)]
            grad = [grad_v[:, a] for a in at]
            level = [jnp.mean(g * n, axis=-1, keepdims=True) for g, n in zip(grad, normed)]
            d_o = [(i * (g - n * m)).astype(BF16) for i, g, n, m in zip(inverse, grad, normed, level)]
            d_prefix = [dot_tn(a, b) for a, b in zip(q, d_o)]
            att = [n.astype(BF16) for n in normed]
            turned = [a.astype(F32).T.astype(BF16).reshape(2, 4, 16, TOK) for a in att]
            for i, j in enumerate(js):
                h = 4 * j + c
                hh = h % 8
                att_v[:, at[i]] = att[i]
                do_v[:, at[i]] = d_o[i]
                state[j, c] = d_prefix[i]
                attT[h // 8, hh // 2, pl.ds(2 * (hh % 2), 2)] = turned[i]
        heads_of(some, c)

    def att_copies(c):
        return [
            send(attS.at[2 * c + i], attR.at[2 * c + i], ats.at[0], atr.at[c], other)
            for i in range(2)
        ]

    @scoped
    def att_give(c):
        for i, copy in enumerate(att_copies(c)):
            hh = 4 * i + c
            attS[2 * c + i] = attT[1 - d, hh // 2, 2 * (hh % 2):2 * (hh % 2) + 2].astype(F32)
            copy.start()

    @scoped
    def att_take(c):
        both = attR.at[2 * c:2 * c + 2]
        send(both, both, ats.at[0], atr.at[c], other).wait_recv()
        for i in range(2):
            hh = 4 * i + c
            attP[hh // 2, 2 * (hh % 2):2 * (hh % 2) + 2] = attR[2 * c + i].astype(BF16)

    forward = (
        (grad_tiles, 0, 4), (1, 0), (grad_tiles, 4, 6), (1, 1), (grad_tiles, 6, 8), (2, 0), (1, 2),
        (inside_heads, 0), (2, 1), (1, 3), (inside_heads, 1), (3, 0), (2, 2), (og_take, 0), (inside_heads, 2),
        (3, 1), (2, 3), (4, 0), (inside_heads, 3), (3, 2), (4, 1), (3, 3), (og_take, 1), (4, 2), (og_take, 2),
        (4, 3),
    )
    loads[3].wait()
    for item in forward:
        if callable(item[0]):
            item[0](*item[1:])
        else:
            scan1.step(*item)
    scan1.drain(0)
    @scoped
    def product(i, t):
        color = colors[i]
        axis = ORDERS[i][0]
        idx = [slice(None)] * 3
        idx[axis] = t
        idx = tuple(idx)
        both = jnp.concatenate([attT[(d,) + idx].reshape(TOK, TOK), attP[idx].reshape(TOK, TOK)], axis=1)
        for low in range(0, WIDTHS[i], COL):
            high = min(low + COL, WIDTHS[i])
            block = dot_nn(both, og_v[:, STARTS[i] + low:STARTS[i] + high])
            color.part[idx + (slice(None), slice(None), slice(low, high))] = block.reshape(4, 4, 2, 8, high - low)

    @scoped
    def backward_heads(c):
        def some(js, c):
            at = [cols(4 * j + c) for j in js]
            q, k, v, d_o = ([ref[:, a] for a in at] for ref in (q_v, k_v, v_v, do_v))
            probs = [jnp.where(lower, dot_nt(a, b), 0.0).astype(BF16) for a, b in zip(q, k)]
            d_probs = [jnp.where(lower, dot_nt(a, b), 0.0).astype(BF16) for a, b in zip(d_o, v)]
            before = [two_parts(r1[j, c]) for j in js]
            after = [two_parts(r2[j, c]) for j in js]
            n = range(len(js))
            q_grad = [dot_nn(d_probs[i], k[i]) + sum(dot_nt(d_o[i], p) for p in before[i]) for i in n]
            k_grad = [dot_tn(d_probs[i], q[i]) + sum(dot_nt(v[i], p) for p in after[i]) for i in n]
            v_grad = [dot_tn(probs[i], d_o[i]) + sum(dot_nn(k[i], p) for p in after[i]) for i in n]
            for i in n:
                q_v[:, at[i]] = q_grad[i].astype(BF16)
                k_v[:, at[i]] = k_grad[i].astype(BF16)
                v_v[:, at[i]] = v_grad[i].astype(BF16)
        heads_of(some, c)

    cz, cx, cy = colors

    def up_down(color, pair, u):
        color.go(0, 2 * pair, u)
        color.go(0, 2 * pair + 1, u)

    def paced(color, pair, u):
        n = 4 * pair + u - 2
        color.left(n // 4, n % 4)
        up_down(color, pair, u)

    def early_and_late(kinds_even, kinds_odd, us):
        for parity, kinds in ((0, kinds_even), (1, kinds_odd)):
            @pl.when(z % 2 == parity)
            def _(kinds=kinds):
                for u in us:
                    for kind in kinds:
                        cz.go(0, kind, u)

    for c in range(N_CHUNK):
        scan1.step(5, c)
        forward_heads(c)
        scan2.step(0, c)
        att_give(c)
        if c == 2:
            og_copy(0).wait_send()
            att_take(0)
            att_take(1)
            product(0, 0)
            product(0, 2)
            early_and_late((0, 1), (2, 3), (0, 1, 2))
    att_take(2)
    att_take(3)
    for i in (1, 2):
        og_copy(i).wait_send()
    product(1, (x + 2) % 4)
    up_down(cx, 0, 0)
    up_down(cx, 0, 1)
    product(2, (y + 2) % 4)
    for u in range(4):
        up_down(cy, 0, u)
    scan2.step(1, 0)
    product(1, (x + 1) % 4)
    product(1, (x + 3) % 4)
    product(2, (y + 1) % 4)
    product(2, (y + 3) % 4)
    up_down(cy, 1, 0)
    up_down(cy, 1, 1)
    scan2.step(1, 1)
    product(0, 1)
    product(0, 3)
    product(1, x)
    product(2, y)
    scan2.step(1, 2)
    scan2.step(1, 3)
    paced(cx, 0, 2)
    scan2.step(2, 0)
    early_and_late((0, 1), (2, 3), (3,))
    scan2.step(2, 1)
    for stage in range(1, 5):
        scan1.drain(stage)
    paced(cx, 0, 3)
    scan2.step(2, 2)
    early_and_late((2, 3), (0, 1), (0,))
    scan2.step(3, 0)
    paced(cx, 1, 0)
    for item in ((2, 3), (3, 1)):
        scan2.step(*item)
    early_and_late((2, 3), (0, 1), (1, 2, 3))
    paced(cx, 1, 1)
    scan2.step(4, 0)
    scan2.step(3, 2)
    paced(cx, 1, 2)
    paced(cy, 1, 2)
    cz.relay(0, 0)
    scan2.step(4, 1)
    scan2.step(3, 3)
    up_down(cx, 1, 3)
    for u in range(4):
        cx.relay(0, u)
    cz.relay(0, 1)
    paced(cy, 1, 3)
    scan2.step(4, 2)
    cy.relay(0, 0)
    cz.relay(0, 2)
    scan2.step(4, 3)
    cz.relay(0, 3)
    for u in range(1, 4):
        cy.relay(0, u)

    def finish_first(color, u):
        color.finish(0, u)
        for v in range(4):
            if u == 0:
                color.go(1, 0, v)
                color.go(1, 1, v)
            elif u < 3:
                color.go(1, 1 + u, v)

    def finish_second(color, v):
        color.finish(1, v)
        if v < 3:
            color.direct((2, 1, 3)[v]).start()

    for u in range(3):
        scan2.step(5, u)
        backward_heads(u)
    finish_first(cx, 0)
    finish_first(cz, 0)
    scan2.step(5, 3)
    backward_heads(3)
    for color, u in (
        (cx, 1), (cy, 0), (cz, 1), (cx, 2), (cy, 1), (cx, 3), (cz, 2), (cy, 2), (cz, 3), (cy, 3)
    ):
        finish_first(color, u)
    for stage in range(5):
        scan2.drain(stage)
    send(attS, attS, ats.at[0], atr.at[0], other).wait_send()
    for color in colors:
        color.drain(0)
    for v in range(4):
        for color in (cx, cz, cy):
            color.relay(1, v)
    for v in range(4):
        for color in (cx, cz, cy):
            finish_second(color, v)
    for color in colors:
        color.drain(1)
    for i in (1, 0, 2):
        colors[i].last(wg_v, STARTS[i], WIDTHS[i])
    for color in colors:
        color.drain(2)


def store_kernel(*refs):
    sources, targets, sems = refs[:5], refs[5:10], refs[10]
    copies = [
        pltpu.make_async_copy(src, dst.at[0] if i < 4 else dst, sems.at[i])
        for i, (src, dst) in enumerate(zip(sources, targets))
    ]
    for copy in copies:
        copy.start()
    for copy in copies:
        copy.wait()


def body(queries, keys, values, out_grad, out_weight):
    vm = pltpu.VMEM
    dma = pltpu.SemaphoreType.DMA

    def scan_bufs():
        return [
            vm((4, 4, 128, 128), F32), vm((4, 4, 32, 128), F32), vm((4, 4, 32, 128), F32),
            vm((4, 32, 128), F32), vm((4, 4, 32, 128), F32), vm((4, 4, 32, 128), F32),
            vm((4, 4, 128, 128), F32),
        ]

    scratch = [
        vm((2 * TOK, D), BF16), vm((W_SLOTS, W_ROWS, D), BF16),
        vm((TOK, HD), F32), vm((TOK, HD), F32), vm((TOK, HD), BF16),
        vm((2, 4, 4, 4, 16, TOK), BF16), vm((4, 4, 4, 16, TOK), BF16),
        vm((8, 2, 4, 16, TOK), F32), vm((8, 2, 4, 16, TOK), F32),
        vm((4, 4, 128, 128), F32),
        *scan_bufs(), *scan_bufs(),
        *[vm((4, 4, 4, 2, 8, w), F32) for w in WIDTHS],
    ]
    scratch += [vm((6, 4, 4, 8, w), F32) for w in WIDTHS]
    scratch += [vm((6, 4, 8, w), F32) for w in WIDTHS]
    scratch += [vm((3, 2, 8, w), F32) for w in WIDTHS]
    scratch += [
        dma((4,)), dma((W_SLOTS,)),
        dma((5,)), dma((4, 5)), dma((5,)), dma((4, 5)),
        dma((3, 14)), dma((3, 18)), dma((3,)), dma((3,)), dma((1,)), dma((4,)),
    ]
    any_space = pl.BlockSpec(memory_space=pl.ANY)
    in_vmem = pl.BlockSpec(memory_space=vm)
    results = pl.pallas_call(
        kernel,
        out_shape=(vm((TOK, HD), BF16),) * 4 + (vm((2, 8, D), F32),),
        in_specs=[any_space] * 5,
        out_specs=(in_vmem,) * 5,
        scratch_shapes=scratch,
        compiler_params=pltpu.CompilerParams(
            collective_id=0, has_side_effects=True, vmem_limit_bytes=VMEM_LIMIT
        ),
        name="block",
    )(queries, keys, values, out_grad, out_weight)
    flat = jax.ShapeDtypeStruct((1, TOK, HD), BF16)
    attended, d_query, d_key, d_value, weight_grad = pl.pallas_call(
        store_kernel,
        out_shape=(flat,) * 4 + (jax.ShapeDtypeStruct((2, 8, D), F32),),
        in_specs=[in_vmem] * 5,
        out_specs=(any_space,) * 5,
        scratch_shapes=[dma((5,))],
        compiler_params=pltpu.CompilerParams(vmem_limit_bytes=1 << 20),
        name="store",
    )(*results)
    return attended, d_query, d_key, d_value, weight_grad.reshape(16, D)


def solution(mesh):
    split = Mesh(mesh.devices.reshape(mesh.shape[DP], 4, 4, 4), DP_SEQ)
    rows = P(DP, SEQ, None)
    return jax.shard_map(
        body, mesh=split, in_specs=(rows, rows, rows, rows, P()),
        out_specs=(rows, rows, rows, rows, P(DP_SEQ, None)), check_vma=False,
    )
```

```python
import functools

import jax
import jax.numpy as jnp
from jax import lax
from jax.experimental import pallas as pl
from jax.experimental.pallas import tpu as pltpu
from jax.sharding import Mesh
from jax.sharding import PartitionSpec as P

P_SIZE = 128
H = 16
HD = 2048
D = 4096
TOK = 256
EPS = 1e-06
F32 = jnp.float32
BF16 = jnp.bfloat16
MESH = pl.DeviceIdType.MESH
DP = "dp"
SEQ = ("seq_0", "seq_1", "seq_2")
DP_SEQ = (DP,) + SEQ
N_CHUNK = 4
WIDTHS = (1536, 1408, 1152)
STARTS = (0, 1536, 2944)
ORDERS = ((0, 1, 2), (1, 2, 0), (2, 0, 1))
COL = 256
W_ROWS = 256
W_TILES = HD // W_ROWS
W_SLOTS = 3
VMEM_LIMIT = 62_500_000


def dot_nn(a, b):
    return lax.dot_general(a, b, (((1,), (0,)), ((), ())), preferred_element_type=F32)


def dot_nt(a, b):
    return lax.dot_general(a, b, (((1,), (1,)), ((), ())), preferred_element_type=F32)


def dot_tn(a, b):
    return lax.dot_general(a, b, (((0,), (0,)), ((), ())), preferred_element_type=F32)


def two_parts(x):
    high = x.astype(BF16)
    return high, (x - high.astype(F32)).astype(BF16)


def send(src, dst, send_sem, recv_sem, device):
    return pltpu.make_async_remote_copy(
        src_ref=src, dst_ref=dst, send_sem=send_sem, recv_sem=recv_sem,
        device_id=device, device_id_type=MESH,
    )


def scoped(f):
    @functools.wraps(f)
    def named(*args):
        with jax.named_scope(f.__name__ + "_" + "".join(str(a) for a in args if isinstance(a, int))):
            return f(*args)
    return named


class Scan:
    def __init__(self, where, bufs, sems, reverse):
        self.z, self.x, self.y = where
        self.S, self.YR, self.T, self.XR, self.PT, self.ZR, self.XC, self.R = bufs
        self.ss, self.rs = sems
        self.reverse = reverse

    def order(self):
        return range(3, -1, -1) if self.reverse else range(4)

    def copies(self, stage, c):
        out = []
        for r in (2, 1, 3):
            s, v = self.ss.at[stage], self.rs.at[c, stage]
            yt, xt, zt = (self.y + r) % 4, (self.x + r) % 4, (self.z + r) % 4
            if stage == 0:
                out.append(send(self.S.at[yt, c], self.YR.at[c, self.y], s, v, {SEQ[2]: yt}))
            elif stage == 1:
                out.append(send(self.T.at[c, xt], self.XR.at[c, self.x], s, v, {SEQ[1]: xt}))
            elif stage == 2:
                out.append(send(self.PT.at[c], self.ZR.at[c, self.z], s, v, {SEQ[0]: zt}))
            elif stage == 3:
                out.append(send(self.XR.at[c, xt], self.XC.at[c, self.x], s, v, {SEQ[1]: xt}))
            else:
                out.append(send(self.YR.at[c, yt], self.R.at[self.y, c], s, v, {SEQ[2]: yt}))
        return out

    def landing(self, stage, c):
        ref = (
            self.YR.at[c, 0:3], self.XR.at[c, 0:3], self.ZR.at[c, 0:3], self.XC.at[c, 0:3], self.R.at[0:3, c]
        )[stage]
        send(ref, ref, self.ss.at[stage], self.rs.at[c, stage], {SEQ[2]: (self.y + 1) % 4}).wait_recv()

    def go(self, stage, c):
        for copy in self.copies(stage, c):
            copy.start()

    def step(self, s, c):
        with jax.named_scope(f"scan{int(self.reverse)}_{s}{c}"):
            self.step_in(s, c)

    def step_in(self, s, c):
        if s > 0:
            self.landing(s - 1, c)
        if s == 0:
            self.YR[c, self.y] = self.S[self.y, c]
        elif s == 1:
            running = None
            for k in self.order():
                now = self.YR[c, k]
                self.YR[c, k] = jnp.zeros_like(now) if running is None else running
                running = now if running is None else running + now
            self.T[c] = running.reshape(4, 32, 128)
            self.XR[c, self.x] = self.T[c, self.x]
        elif s == 2:
            running = None
            for k in self.order():
                now = self.XR[c, k]
                self.XR[c, k] = jnp.zeros_like(now) if running is None else running
                running = now if running is None else running + now
            self.PT[c] = running
            self.ZR[c, self.z] = running
        elif s == 3:
            base = jnp.zeros((32, 128), F32)
            for k in range(4):
                passed = (self.z < k) if self.reverse else (self.z > k)
                base = base + jnp.where(passed, self.ZR[c, k], 0.0)
            for k in range(4):
                self.XR[c, k] = self.XR[c, k] + base
            self.XC[c, self.x] = self.XR[c, self.x]
        elif s == 4:
            carry = self.XC[c].reshape(128, 128)
            for k in range(4):
                self.YR[c, k] = self.YR[c, k] + carry
            self.R[self.y, c] = self.YR[c, self.y]
        if s < 5:
            self.go(s, c)

    def drain(self, stage):
        ref = (self.S.at[0:3], self.T.at[:, 0:3], self.T.at[:, 0:3], self.T.at[:, 0:3], self.S.at[0:3])[stage]
        send(ref, ref, self.ss.at[stage], self.rs.at[0, stage], {SEQ[2]: (self.y + 1) % 4}).wait_send()


class Color:
    def __init__(self, where, order, part, recv, ss, rs):
        self.where, self.order, self.part, self.recv, self.ss, self.rs = where, order, part, recv, ss, rs
        self.gone = set()

    def axis(self, phase):
        return self.order[phase]

    def slot(self, phase, t, u):
        idx = [slice(None)] * 3
        for p in range(phase):
            idx[self.order[p]] = self.where[self.order[p]]
        idx[self.order[phase]] = t
        if phase < 2:
            nxt = self.order[phase + 1]
            idx[nxt] = (self.where[nxt] + (2, 1, 3, 0)[u]) % 4
        return idx

    def sems(self, phase, kind, u):
        leave = 4 * (kind // 2) + u if phase == 0 else 11 + phase
        land = 8 * phase + 2 * u + (0 if kind < 2 else 1)
        return self.ss.at[leave], self.rs.at[land]

    def copy(self, phase, kind, u=0):
        a = self.axis(phase)
        m = self.where[a]
        up = kind % 2 == 0
        to = (m + 1) % 4 if up else (m + 3) % 4
        t = (m + 2) % 4 if kind < 2 else to
        half = (0, 1, 1, 0, 0, 1)[kind]
        src = self.part.at[tuple(self.slot(phase, t, u)) + (half,)]
        dst = self.recv[phase].at[kind, u]
        return send(src, dst, *self.sems(phase, kind, u), {SEQ[a]: to})

    def go(self, phase, kind, u=0):
        self.copy(phase, kind, u).start()

    def bulk(self, phase, kinds, u, ref):
        a = self.axis(phase)
        return send(ref, ref, *self.sems(phase, kinds.start, u), {SEQ[a]: (self.where[a] + 1) % 4})

    def left(self, pair, u):
        if (pair, u) not in self.gone:
            self.gone.add((pair, u))
            kinds = slice(2 * pair, 2 * pair + 2)
            self.bulk(0, kinds, u, self.recv[0].at[kinds, u]).wait_send()

    def landed(self, phase, kinds, u):
        self.bulk(phase, kinds, u, self.recv[phase].at[kinds, u]).wait_recv()

    def got(self, phase, kind, u=0):
        return self.recv[phase][kind, u]

    def relay(self, phase, u=0):
        with jax.named_scope(f"relay{self.order[0]}_{phase}{u}"):
            self.relay_in(phase, u)

    def relay_in(self, phase, u=0):
        m = self.where[self.axis(phase)]
        self.landed(phase, slice(0, 2), u)
        for kind, to, half in ((0, (m + 1) % 4, 0), (1, (m + 3) % 4, 1)):
            more = self.got(phase, kind, u)
            at = tuple(self.slot(phase, to, u)) + (half,)
            self.part[at] = self.part[at] + more
            self.go(phase, 4 + kind, u)

    def finish(self, phase, u=0):
        with jax.named_scope(f"finish{self.order[0]}_{phase}{u}"):
            self.finish_in(phase, u)

    def finish_in(self, phase, u=0):
        m = self.where[self.axis(phase)]
        self.landed(phase, slice(2, 6), u)
        for half, kinds in ((0, (3, 4)), (1, (2, 5))):
            more = self.got(phase, kinds[0], u) + self.got(phase, kinds[1], u)
            at = tuple(self.slot(phase, m, u)) + (half,)
            self.part[at] = self.part[at] + more

    def direct(self, r):
        a = self.axis(2)
        to = (self.where[a] + r) % 4
        src = self.part.at[tuple(self.slot(2, to, 0))]
        return send(src, self.recv[2].at[r - 1], *self.sems(2, 0, 0), {SEQ[a]: to})

    def last(self, out, start, width):
        with jax.named_scope(f"last{self.order[0]}"):
            self.bulk(2, slice(0, 6), 0, self.recv[2]).wait_recv()
            own = self.part[tuple(self.slot(2, self.where[self.axis(2)], 0))]
            total = (own + self.recv[2][0]) + (self.recv[2][1] + self.recv[2][2])
            out[:, :, start:start + width] = total

    def drain(self, phase):
        if phase == 0:
            for pair in range(3):
                for u in range(4):
                    self.left(pair, u)
        else:
            self.bulk(phase, slice(0, 6), 0, self.recv[phase]).wait_send()


def kernel(
    q_hbm, k_hbm, v_hbm, og_hbm, w_hbm,
    att_v, q_v, k_v, v_v, wg_v,
    og_v, w_v, grad_v, intra_v, do_v, attT, attP, attS, attR,
    state, yr1, t1, xr1, pt1, zr1, xc1, r1,
    yr2, t2, xr2, pt2, zr2, xc2, r2,
    p0, p1, p2, a0, a1, a2, b0, b1, b2, c0, c1, c2,
    in_sem, w_sem, s1s, s1r, s2s, s2r, css, crs, ogs, ogr, ats, atr,
):
    d = lax.axis_index(DP)
    where = tuple(lax.axis_index(a) for a in SEQ)
    z, x, y = where
    other = {DP: 1 - d}
    parts = (p0, p1, p2)

    loads = [
        pltpu.make_async_copy(src.at[0], dst, in_sem.at[i])
        for i, (src, dst) in enumerate(((k_hbm, k_v), (v_hbm, v_v), (og_hbm, og_v.at[:TOK]), (q_hbm, q_v)))
    ]
    loads[0].start()
    loads[1].start()

    def w_load(i):
        return pltpu.make_async_copy(
            w_hbm.at[pl.ds(pl.multiple_of(i * W_ROWS, W_ROWS), W_ROWS)], w_v.at[i % W_SLOTS], w_sem.at[i % W_SLOTS]
        )

    barrier = pltpu.get_barrier_semaphore()
    pl.semaphore_signal(barrier, inc=1, device_id=other, device_id_type=MESH)
    for a in range(3):
        for r in range(1, 4):
            pl.semaphore_signal(barrier, inc=1, device_id={SEQ[a]: (where[a] + r) % 4}, device_id_type=MESH)

    scan1 = Scan(where, (state, yr1, t1, xr1, pt1, zr1, xc1, r1), (s1s, s1r), False)
    scan2 = Scan(where, (state, yr2, t2, xr2, pt2, zr2, xc2, r2), (s2s, s2r), True)
    colors = [
        Color(where, ORDERS[i], parts[i], ((a0, b0, c0), (a1, b1, c1), (a2, b2, c2))[i], css.at[i], crs.at[i])
        for i in range(3)
    ]

    def cols(h):
        return pl.ds(pl.multiple_of(h * P_SIZE, P_SIZE), P_SIZE)

    def heads_of(fn, c, width=2):
        def one(n, carry):
            fn([n * width + i for i in range(width)], c)
            return carry
        lax.fori_loop(0, 4 // width, one, 0)

    @scoped
    def states(c):
        def some(js, c):
            at = [cols(4 * j + c) for j in js]
            out = [dot_tn(k_v[:, a], v_v[:, a]) for a in at]
            for j, value in zip(js, out):
                state[j, c] = value
        heads_of(some, c)

    with jax.named_scope("load"):
        loads[0].wait()
        loads[1].wait()
    loads[2].start()
    for i in range(W_SLOTS):
        w_load(i).start()
    loads[3].start()
    states(0)
    with jax.named_scope("enter"):
        pl.semaphore_wait(barrier, 10)
    scan1.step(0, 0)
    for c in range(1, N_CHUNK):
        states(c)
        scan1.step(0, c)

    loads[2].wait()

    def og_copy(i):
        return send(parts[i].at[0], parts[i].at[1], ogs.at[i], ogr.at[i], other)

    for i in range(3):
        def put(n, carry, i=i):
            rows = pl.ds(pl.multiple_of(n * 64, 64), 64)
            block = og_v[rows, STARTS[i]:STARTS[i] + WIDTHS[i]].astype(F32)
            parts[i][0, n] = block.reshape(4, 2, 8, WIDTHS[i])
            return carry
        lax.fori_loop(0, 4, put, 0)
        og_copy(i).start()

    @scoped
    def grad_tiles(lo, hi):
        def one(i, carry):
            w_load(i).wait()
            block = dot_nt(og_v[:TOK], w_v[i % W_SLOTS])
            at = pl.ds(pl.multiple_of(i * W_ROWS, W_ROWS), W_ROWS)
            grad_v[:, at] = block

            @pl.when(i + W_SLOTS < W_TILES)
            def _():
                w_load(i + W_SLOTS).start()
            return carry
        lax.fori_loop(lo, hi, one, 0)

    @scoped
    def og_take(i):
        og_copy(i).wait_recv()
        def take(n, carry):
            rows = pl.ds(pl.multiple_of(TOK + n * 64, 64), 64)
            block = parts[i][1, n].reshape(64, WIDTHS[i])
            og_v[rows, STARTS[i]:STARTS[i] + WIDTHS[i]] = block.astype(BF16)
            return carry
        lax.fori_loop(0, 4, take, 0)

    lower = (
        lax.broadcasted_iota(jnp.int32, (TOK, TOK), 0) >= lax.broadcasted_iota(jnp.int32, (TOK, TOK), 1)
    )

    @scoped
    def inside_heads(c):
        def some(js, c):
            at = [cols(4 * j + c) for j in js]
            scores = [dot_nt(q_v[:, a], k_v[:, a]) for a in at]
            probs = [jnp.where(lower, x, 0.0).astype(BF16) for x in scores]
            out = [dot_nn(p, v_v[:, a]) for p, a in zip(probs, at)]
            for a, value in zip(at, out):
                intra_v[:, a] = value
        heads_of(some, c)

    @scoped
    def forward_heads(c):
        def some(js, c):
            at = [cols(4 * j + c) for j in js]
            q = [q_v[:, a] for a in at]
            split = [two_parts(r1[j, c]) for j in js]
            inter = [dot_nn(a, high) + dot_nn(a, low) for a, (high, low) in zip(q, split)]
            o = [intra_v[:, a] + x for a, x in zip(at, inter)]
            inverse = [lax.rsqrt(jnp.mean(x * x, axis=-1, keepdims=True) + EPS) for x in o]
            normed = [x * i for x, i in zip(o, inverse)]
            grad = [grad_v[:, a] for a in at]
            level = [jnp.mean(g * n, axis=-1, keepdims=True) for g, n in zip(grad, normed)]
            d_o = [(i * (g - n * m)).astype(BF16) for i, g, n, m in zip(inverse, grad, normed, level)]
            d_prefix = [dot_tn(a, b) for a, b in zip(q, d_o)]
            att = [n.astype(BF16) for n in normed]
            turned = [a.astype(F32).T.astype(BF16).reshape(2, 4, 16, TOK) for a in att]
            for i, j in enumerate(js):
                h = 4 * j + c
                hh = h % 8
                att_v[:, at[i]] = att[i]
                do_v[:, at[i]] = d_o[i]
                state[j, c] = d_prefix[i]
                attT[h // 8, hh // 2, pl.ds(2 * (hh % 2), 2)] = turned[i]
        heads_of(some, c)

    def att_copies(c):
        return [
            send(attS.at[2 * c + i], attR.at[2 * c + i], ats.at[0], atr.at[c], other)
            for i in range(2)
        ]

    @scoped
    def att_give(c):
        for i, copy in enumerate(att_copies(c)):
            hh = 4 * i + c
            attS[2 * c + i] = attT[1 - d, hh // 2, 2 * (hh % 2):2 * (hh % 2) + 2].astype(F32)
            copy.start()

    @scoped
    def att_take(c):
        both = attR.at[2 * c:2 * c + 2]
        send(both, both, ats.at[0], atr.at[c], other).wait_recv()
        for i in range(2):
            hh = 4 * i + c
            attP[hh // 2, 2 * (hh % 2):2 * (hh % 2) + 2] = attR[2 * c + i].astype(BF16)

    forward = (
        (grad_tiles, 0, 4), (1, 0), (grad_tiles, 4, 6), (1, 1), (grad_tiles, 6, 8), (2, 0), (1, 2),
        (inside_heads, 0), (2, 1), (1, 3), (inside_heads, 1), (3, 0), (2, 2), (og_take, 0), (inside_heads, 2),
        (3, 1), (2, 3), (4, 0), (inside_heads, 3), (3, 2), (4, 1), (3, 3), (og_take, 1), (4, 2), (og_take, 2),
        (4, 3),
    )
    loads[3].wait()
    for item in forward:
        if callable(item[0]):
            item[0](*item[1:])
        else:
            scan1.step(*item)
    scan1.drain(0)
    @scoped
    def product(i, t):
        color = colors[i]
        axis = ORDERS[i][0]
        idx = [slice(None)] * 3
        idx[axis] = t
        idx = tuple(idx)
        both = jnp.concatenate([attT[(d,) + idx].reshape(TOK, TOK), attP[idx].reshape(TOK, TOK)], axis=1)
        for low in range(0, WIDTHS[i], COL):
            high = min(low + COL, WIDTHS[i])
            block = dot_nn(both, og_v[:, STARTS[i] + low:STARTS[i] + high])
            color.part[idx + (slice(None), slice(None), slice(low, high))] = block.reshape(4, 4, 2, 8, high - low)

    @scoped
    def backward_heads(c):
        def some(js, c):
            at = [cols(4 * j + c) for j in js]
            q, k, v, d_o = ([ref[:, a] for a in at] for ref in (q_v, k_v, v_v, do_v))
            probs = [jnp.where(lower, dot_nt(a, b), 0.0).astype(BF16) for a, b in zip(q, k)]
            d_probs = [jnp.where(lower, dot_nt(a, b), 0.0).astype(BF16) for a, b in zip(d_o, v)]
            before = [two_parts(r1[j, c]) for j in js]
            after = [two_parts(r2[j, c]) for j in js]
            n = range(len(js))
            q_grad = [dot_nn(d_probs[i], k[i]) + sum(dot_nt(d_o[i], p) for p in before[i]) for i in n]
            k_grad = [dot_tn(d_probs[i], q[i]) + sum(dot_nt(v[i], p) for p in after[i]) for i in n]
            v_grad = [dot_tn(probs[i], d_o[i]) + sum(dot_nn(k[i], p) for p in after[i]) for i in n]
            for i in n:
                q_v[:, at[i]] = q_grad[i].astype(BF16)
                k_v[:, at[i]] = k_grad[i].astype(BF16)
                v_v[:, at[i]] = v_grad[i].astype(BF16)
        heads_of(some, c)

    cz, cx, cy = colors

    def up_down(color, pair, u):
        color.go(0, 2 * pair, u)
        color.go(0, 2 * pair + 1, u)

    def paced(color, pair, u):
        n = 4 * pair + u - 2
        color.left(n // 4, n % 4)
        up_down(color, pair, u)

    def early_and_late(kinds_even, kinds_odd, us):
        for parity, kinds in ((0, kinds_even), (1, kinds_odd)):
            @pl.when(z % 2 == parity)
            def _(kinds=kinds):
                for u in us:
                    for kind in kinds:
                        cz.go(0, kind, u)

    for c in range(N_CHUNK):
        scan1.step(5, c)
        forward_heads(c)
        scan2.step(0, c)
        att_give(c)
        if c == 2:
            og_copy(0).wait_send()
            att_take(0)
            att_take(1)
            product(0, 0)
            product(0, 2)
            early_and_late((0, 1), (2, 3), (0, 1, 2))
    att_take(2)
    att_take(3)
    for i in (1, 2):
        og_copy(i).wait_send()
    product(1, (x + 2) % 4)
    up_down(cx, 0, 0)
    up_down(cx, 0, 1)
    product(2, (y + 2) % 4)
    for u in range(4):
        up_down(cy, 0, u)
    scan2.step(1, 0)
    product(1, (x + 1) % 4)
    product(1, (x + 3) % 4)
    product(2, (y + 1) % 4)
    product(2, (y + 3) % 4)
    up_down(cy, 1, 0)
    up_down(cy, 1, 1)
    scan2.step(1, 1)
    product(0, 1)
    product(0, 3)
    product(1, x)
    product(2, y)
    scan2.step(1, 2)
    scan2.step(1, 3)
    paced(cx, 0, 2)
    scan2.step(2, 0)
    early_and_late((0, 1), (2, 3), (3,))
    scan2.step(2, 1)
    for stage in range(1, 5):
        scan1.drain(stage)
    paced(cx, 0, 3)
    scan2.step(2, 2)
    early_and_late((2, 3), (0, 1), (0,))
    scan2.step(3, 0)
    paced(cx, 1, 0)
    for item in ((2, 3), (3, 1)):
        scan2.step(*item)
    early_and_late((2, 3), (0, 1), (1, 2, 3))
    paced(cx, 1, 1)
    scan2.step(4, 0)
    scan2.step(3, 2)
    paced(cx, 1, 2)
    paced(cy, 1, 2)
    cz.relay(0, 0)
    scan2.step(4, 1)
    scan2.step(3, 3)
    up_down(cx, 1, 3)
    for u in range(4):
        cx.relay(0, u)
    paced(cy, 1, 3)
    scan2.step(4, 2)
    cy.relay(0, 0)
    scan2.step(4, 3)
    for u in range(1, 4):
        cy.relay(0, u)
    cz.relay(0, 1)
    cz.relay(0, 2)

    def finish_first(color, u):
        color.finish(0, u)
        if u == 0:
            for v in range(4):
                color.go(1, 0, v)
                color.go(1, 1, v)
        elif u < 3:
            color.go(1, 1 + u, 0)

    def finish_second(color, v):
        color.finish(1, v)
        if v < 3:
            color.direct((2, 1, 3)[v]).start()

    for u in range(3):
        scan2.step(5, u)
        backward_heads(u)
        if u == 0:
            cz.relay(0, 3)
    finish_first(cx, 0)
    finish_first(cz, 0)
    scan2.step(5, 3)
    backward_heads(3)
    for color, u in (
        (cx, 1), (cy, 0), (cz, 1), (cx, 2), (cy, 1), (cx, 3), (cz, 2), (cy, 2), (cz, 3), (cy, 3)
    ):
        finish_first(color, u)
    for stage in range(5):
        scan2.drain(stage)
    send(attS, attS, ats.at[0], atr.at[0], other).wait_send()
    for color in colors:
        color.drain(0)
    for v in range(4):
        for color in (cx, cz, cy):
            color.relay(1, v)
            if v < 3:
                color.go(1, 2, v + 1)
                color.go(1, 3, v + 1)
    for v in range(4):
        for color in (cx, cz, cy):
            finish_second(color, v)
    for color in colors:
        color.drain(1)
    for i in (1, 0, 2):
        colors[i].last(wg_v, STARTS[i], WIDTHS[i])
    for color in colors:
        color.drain(2)


def store_kernel(*refs):
    sources, targets, sems = refs[:5], refs[5:10], refs[10]
    copies = [
        pltpu.make_async_copy(src, dst.at[0] if i < 4 else dst, sems.at[i])
        for i, (src, dst) in enumerate(zip(sources, targets))
    ]
    for copy in copies:
        copy.start()
    for copy in copies:
        copy.wait()


def body(queries, keys, values, out_grad, out_weight):
    vm = pltpu.VMEM
    dma = pltpu.SemaphoreType.DMA

    def scan_bufs():
        return [
            vm((4, 4, 128, 128), F32), vm((4, 4, 32, 128), F32), vm((4, 4, 32, 128), F32),
            vm((4, 32, 128), F32), vm((4, 4, 32, 128), F32), vm((4, 4, 32, 128), F32),
            vm((4, 4, 128, 128), F32),
        ]

    scratch = [
        vm((2 * TOK, D), BF16), vm((W_SLOTS, W_ROWS, D), BF16),
        vm((TOK, HD), F32), vm((TOK, HD), F32), vm((TOK, HD), BF16),
        vm((2, 4, 4, 4, 16, TOK), BF16), vm((4, 4, 4, 16, TOK), BF16),
        vm((8, 2, 4, 16, TOK), F32), vm((8, 2, 4, 16, TOK), F32),
        vm((4, 4, 128, 128), F32),
        *scan_bufs(), *scan_bufs(),
        *[vm((4, 4, 4, 2, 8, w), F32) for w in WIDTHS],
    ]
    scratch += [vm((6, 4, 4, 8, w), F32) for w in WIDTHS]
    scratch += [vm((6, 4, 8, w), F32) for w in WIDTHS]
    scratch += [vm((3, 2, 8, w), F32) for w in WIDTHS]
    scratch += [
        dma((4,)), dma((W_SLOTS,)),
        dma((5,)), dma((4, 5)), dma((5,)), dma((4, 5)),
        dma((3, 14)), dma((3, 18)), dma((3,)), dma((3,)), dma((1,)), dma((4,)),
    ]
    any_space = pl.BlockSpec(memory_space=pl.ANY)
    in_vmem = pl.BlockSpec(memory_space=vm)
    results = pl.pallas_call(
        kernel,
        out_shape=(vm((TOK, HD), BF16),) * 4 + (vm((2, 8, D), F32),),
        in_specs=[any_space] * 5,
        out_specs=(in_vmem,) * 5,
        scratch_shapes=scratch,
        compiler_params=pltpu.CompilerParams(
            collective_id=0, has_side_effects=True, vmem_limit_bytes=VMEM_LIMIT
        ),
        name="block",
    )(queries, keys, values, out_grad, out_weight)
    flat = jax.ShapeDtypeStruct((1, TOK, HD), BF16)
    attended, d_query, d_key, d_value, weight_grad = pl.pallas_call(
        store_kernel,
        out_shape=(flat,) * 4 + (jax.ShapeDtypeStruct((2, 8, D), F32),),
        in_specs=[in_vmem] * 5,
        out_specs=(any_space,) * 5,
        scratch_shapes=[dma((5,))],
        compiler_params=pltpu.CompilerParams(vmem_limit_bytes=1 << 20),
        name="store",
    )(*results)
    return attended, d_query, d_key, d_value, weight_grad.reshape(16, D)


def solution(mesh):
    split = Mesh(mesh.devices.reshape(mesh.shape[DP], 4, 4, 4), DP_SEQ)
    rows = P(DP, SEQ, None)
    return jax.shard_map(
        body, mesh=split, in_specs=(rows, rows, rows, rows, P()),
        out_specs=(rows, rows, rows, rows, P(DP_SEQ, None)), check_vma=False,
    )
```

```python
import functools

import jax
import jax.numpy as jnp
from jax import lax
from jax.experimental import pallas as pl
from jax.experimental.pallas import tpu as pltpu
from jax.sharding import Mesh
from jax.sharding import PartitionSpec as P

P_SIZE = 128
H = 16
HD = 2048
D = 4096
TOK = 256
EPS = 1e-06
F32 = jnp.float32
BF16 = jnp.bfloat16
MESH = pl.DeviceIdType.MESH
DP = "dp"
SEQ = ("seq_0", "seq_1", "seq_2")
DP_SEQ = (DP,) + SEQ
N_CHUNK = 4
WIDTHS = (1536, 1408, 1152)
STARTS = (0, 1536, 2944)
ORDERS = ((0, 1, 2), (1, 2, 0), (2, 0, 1))
COL = 256
W_ROWS = 256
W_TILES = HD // W_ROWS
W_SLOTS = 3
VMEM_LIMIT = 62_500_000


def dot_nn(a, b):
    return lax.dot_general(a, b, (((1,), (0,)), ((), ())), preferred_element_type=F32)


def dot_nt(a, b):
    return lax.dot_general(a, b, (((1,), (1,)), ((), ())), preferred_element_type=F32)


def dot_tn(a, b):
    return lax.dot_general(a, b, (((0,), (0,)), ((), ())), preferred_element_type=F32)


def two_parts(x):
    high = x.astype(BF16)
    return high, (x - high.astype(F32)).astype(BF16)


def send(src, dst, send_sem, recv_sem, device):
    return pltpu.make_async_remote_copy(
        src_ref=src, dst_ref=dst, send_sem=send_sem, recv_sem=recv_sem,
        device_id=device, device_id_type=MESH,
    )


def scoped(f):
    @functools.wraps(f)
    def named(*args):
        with jax.named_scope(f.__name__ + "_" + "".join(str(a) for a in args if isinstance(a, int))):
            return f(*args)
    return named


class Scan:
    def __init__(self, where, bufs, sems, reverse):
        self.z, self.x, self.y = where
        self.S, self.YR, self.T, self.XR, self.PT, self.ZR, self.XC, self.R = bufs
        self.ss, self.rs = sems
        self.reverse = reverse

    def order(self):
        return range(3, -1, -1) if self.reverse else range(4)

    def copies(self, stage, c):
        out = []
        for r in (2, 1, 3):
            s, v = self.ss.at[stage], self.rs.at[c, stage]
            yt, xt, zt = (self.y + r) % 4, (self.x + r) % 4, (self.z + r) % 4
            if stage == 0:
                out.append(send(self.S.at[yt, c], self.YR.at[c, self.y], s, v, {SEQ[2]: yt}))
            elif stage == 1:
                out.append(send(self.T.at[c, xt], self.XR.at[c, self.x], s, v, {SEQ[1]: xt}))
            elif stage == 2:
                out.append(send(self.PT.at[c], self.ZR.at[c, self.z], s, v, {SEQ[0]: zt}))
            elif stage == 3:
                out.append(send(self.XR.at[c, xt], self.XC.at[c, self.x], s, v, {SEQ[1]: xt}))
            else:
                out.append(send(self.YR.at[c, yt], self.R.at[self.y, c], s, v, {SEQ[2]: yt}))
        return out

    def landing(self, stage, c):
        ref = (
            self.YR.at[c, 0:3], self.XR.at[c, 0:3], self.ZR.at[c, 0:3], self.XC.at[c, 0:3], self.R.at[0:3, c]
        )[stage]
        send(ref, ref, self.ss.at[stage], self.rs.at[c, stage], {SEQ[2]: (self.y + 1) % 4}).wait_recv()

    def go(self, stage, c):
        for copy in self.copies(stage, c):
            copy.start()

    def step(self, s, c):
        with jax.named_scope(f"scan{int(self.reverse)}_{s}{c}"):
            self.step_in(s, c)

    def step_in(self, s, c):
        if s > 0:
            self.landing(s - 1, c)
        if s == 0:
            self.YR[c, self.y] = self.S[self.y, c]
        elif s == 1:
            running = None
            for k in self.order():
                now = self.YR[c, k]
                self.YR[c, k] = jnp.zeros_like(now) if running is None else running
                running = now if running is None else running + now
            self.T[c] = running.reshape(4, 32, 128)
            self.XR[c, self.x] = self.T[c, self.x]
        elif s == 2:
            running = None
            for k in self.order():
                now = self.XR[c, k]
                self.XR[c, k] = jnp.zeros_like(now) if running is None else running
                running = now if running is None else running + now
            self.PT[c] = running
            self.ZR[c, self.z] = running
        elif s == 3:
            base = jnp.zeros((32, 128), F32)
            for k in range(4):
                passed = (self.z < k) if self.reverse else (self.z > k)
                base = base + jnp.where(passed, self.ZR[c, k], 0.0)
            for k in range(4):
                self.XR[c, k] = self.XR[c, k] + base
            self.XC[c, self.x] = self.XR[c, self.x]
        elif s == 4:
            carry = self.XC[c].reshape(128, 128)
            for k in range(4):
                self.YR[c, k] = self.YR[c, k] + carry
            self.R[self.y, c] = self.YR[c, self.y]
        if s < 5:
            self.go(s, c)

    def drain(self, stage):
        ref = (self.S.at[0:3], self.T.at[:, 0:3], self.T.at[:, 0:3], self.T.at[:, 0:3], self.S.at[0:3])[stage]
        send(ref, ref, self.ss.at[stage], self.rs.at[0, stage], {SEQ[2]: (self.y + 1) % 4}).wait_send()


class Color:
    def __init__(self, where, order, part, recv, ss, rs):
        self.where, self.order, self.part, self.recv, self.ss, self.rs = where, order, part, recv, ss, rs
        self.gone = set()

    def axis(self, phase):
        return self.order[phase]

    def slot(self, phase, t, u):
        idx = [slice(None)] * 3
        for p in range(phase):
            idx[self.order[p]] = self.where[self.order[p]]
        idx[self.order[phase]] = t
        if phase < 2:
            nxt = self.order[phase + 1]
            idx[nxt] = (self.where[nxt] + (2, 1, 3, 0)[u]) % 4
        return idx

    def sems(self, phase, kind, u):
        leave = 4 * (kind // 2) + u if phase == 0 else 11 + phase
        land = 8 * phase + 2 * u + (0 if kind < 2 else 1)
        return self.ss.at[leave], self.rs.at[land]

    def copy(self, phase, kind, u=0):
        a = self.axis(phase)
        m = self.where[a]
        up = kind % 2 == 0
        to = (m + 1) % 4 if up else (m + 3) % 4
        t = (m + 2) % 4 if kind < 2 else to
        half = (0, 1, 1, 0, 0, 1)[kind]
        src = self.part.at[tuple(self.slot(phase, t, u)) + (half,)]
        dst = self.recv[phase].at[kind, u]
        return send(src, dst, *self.sems(phase, kind, u), {SEQ[a]: to})

    def go(self, phase, kind, u=0):
        self.copy(phase, kind, u).start()

    def bulk(self, phase, kinds, u, ref):
        a = self.axis(phase)
        return send(ref, ref, *self.sems(phase, kinds.start, u), {SEQ[a]: (self.where[a] + 1) % 4})

    def left(self, pair, u):
        if (pair, u) not in self.gone:
            self.gone.add((pair, u))
            kinds = slice(2 * pair, 2 * pair + 2)
            self.bulk(0, kinds, u, self.recv[0].at[kinds, u]).wait_send()

    def landed(self, phase, kinds, u):
        self.bulk(phase, kinds, u, self.recv[phase].at[kinds, u]).wait_recv()

    def got(self, phase, kind, u=0):
        return self.recv[phase][kind, u]

    def relay(self, phase, u=0):
        with jax.named_scope(f"relay{self.order[0]}_{phase}{u}"):
            self.relay_in(phase, u)

    def relay_in(self, phase, u=0):
        m = self.where[self.axis(phase)]
        self.landed(phase, slice(0, 2), u)
        for kind, to, half in ((0, (m + 1) % 4, 0), (1, (m + 3) % 4, 1)):
            more = self.got(phase, kind, u)
            at = tuple(self.slot(phase, to, u)) + (half,)
            self.part[at] = self.part[at] + more
            self.go(phase, 4 + kind, u)

    def finish(self, phase, u=0):
        with jax.named_scope(f"finish{self.order[0]}_{phase}{u}"):
            self.finish_in(phase, u)

    def finish_in(self, phase, u=0):
        m = self.where[self.axis(phase)]
        self.landed(phase, slice(2, 6), u)
        for half, kinds in ((0, (3, 4)), (1, (2, 5))):
            more = self.got(phase, kinds[0], u) + self.got(phase, kinds[1], u)
            at = tuple(self.slot(phase, m, u)) + (half,)
            self.part[at] = self.part[at] + more

    def direct(self, r):
        a = self.axis(2)
        to = (self.where[a] + r) % 4
        src = self.part.at[tuple(self.slot(2, to, 0))]
        return send(src, self.recv[2].at[r - 1], *self.sems(2, 0, 0), {SEQ[a]: to})

    def last(self, out, start, width):
        with jax.named_scope(f"last{self.order[0]}"):
            self.bulk(2, slice(0, 6), 0, self.recv[2]).wait_recv()
            own = self.part[tuple(self.slot(2, self.where[self.axis(2)], 0))]
            total = (own + self.recv[2][0]) + (self.recv[2][1] + self.recv[2][2])
            out[:, :, start:start + width] = total

    def drain(self, phase):
        if phase == 0:
            for pair in range(3):
                for u in range(4):
                    self.left(pair, u)
        else:
            self.bulk(phase, slice(0, 6), 0, self.recv[phase]).wait_send()


def kernel(
    q_hbm, k_hbm, v_hbm, og_hbm, w_hbm,
    att_v, q_v, k_v, v_v, wg_v,
    og_v, w_v, grad_v, intra_v, do_v, attT, attP, attS, attR,
    state, yr1, t1, xr1, pt1, zr1, xc1, r1,
    yr2, t2, xr2, pt2, zr2, xc2, r2,
    p0, p1, p2, a0, a1, a2, b0, b1, b2, c0, c1, c2,
    in_sem, w_sem, s1s, s1r, s2s, s2r, css, crs, ogs, ogr, ats, atr,
):
    d = lax.axis_index(DP)
    where = tuple(lax.axis_index(a) for a in SEQ)
    z, x, y = where
    other = {DP: 1 - d}
    parts = (p0, p1, p2)

    loads = [
        pltpu.make_async_copy(src.at[0], dst, in_sem.at[i])
        for i, (src, dst) in enumerate(((og_hbm, og_v.at[:TOK]), (q_hbm, q_v)))
    ]
    for first, size, sem in ((0, P_SIZE, 2), (P_SIZE, 3 * P_SIZE, 3)):
        for j in range(4):
            at = slice(4 * j * P_SIZE + first, 4 * j * P_SIZE + first + size)
            for src, dst in ((k_hbm, k_v), (v_hbm, v_v)):
                pltpu.make_async_copy(src.at[0, :, at], dst.at[:, at], in_sem.at[sem]).start()

    def w_load(i):
        return pltpu.make_async_copy(
            w_hbm.at[pl.ds(pl.multiple_of(i * W_ROWS, W_ROWS), W_ROWS)], w_v.at[i % W_SLOTS], w_sem.at[i % W_SLOTS]
        )

    barrier = pltpu.get_barrier_semaphore()
    pl.semaphore_signal(barrier, inc=1, device_id=other, device_id_type=MESH)
    for a in range(3):
        for r in range(1, 4):
            pl.semaphore_signal(barrier, inc=1, device_id={SEQ[a]: (where[a] + r) % 4}, device_id_type=MESH)

    scan1 = Scan(where, (state, yr1, t1, xr1, pt1, zr1, xc1, r1), (s1s, s1r), False)
    scan2 = Scan(where, (state, yr2, t2, xr2, pt2, zr2, xc2, r2), (s2s, s2r), True)
    colors = [
        Color(where, ORDERS[i], parts[i], ((a0, b0, c0), (a1, b1, c1), (a2, b2, c2))[i], css.at[i], crs.at[i])
        for i in range(3)
    ]

    def cols(h):
        return pl.ds(pl.multiple_of(h * P_SIZE, P_SIZE), P_SIZE)

    def heads_of(fn, c, width=2):
        def one(n, carry):
            fn([n * width + i for i in range(width)], c)
            return carry
        lax.fori_loop(0, 4 // width, one, 0)

    @scoped
    def states(c):
        def some(js, c):
            at = [cols(4 * j + c) for j in js]
            out = [dot_tn(k_v[:, a], v_v[:, a]) for a in at]
            for j, value in zip(js, out):
                state[j, c] = value
        heads_of(some, c)

    with jax.named_scope("load"):
        some = k_v.at[:, :HD // 2]
        pltpu.make_async_copy(some, some, in_sem.at[2]).wait()
    loads[0].start()
    for i in range(W_SLOTS):
        w_load(i).start()
    loads[1].start()
    states(0)
    with jax.named_scope("enter"):
        pl.semaphore_wait(barrier, 10)
    scan1.step(0, 0)
    rest = grad_v.at[:192]
    pltpu.make_async_copy(rest, rest, in_sem.at[3]).wait()
    for c in range(1, N_CHUNK):
        states(c)
        scan1.step(0, c)

    loads[0].wait()

    def og_copy(i):
        return send(parts[i].at[0], parts[i].at[1], ogs.at[i], ogr.at[i], other)

    for i in range(3):
        def put(n, carry, i=i):
            rows = pl.ds(pl.multiple_of(n * 64, 64), 64)
            block = og_v[rows, STARTS[i]:STARTS[i] + WIDTHS[i]].astype(F32)
            parts[i][0, n] = block.reshape(4, 2, 8, WIDTHS[i])
            return carry
        lax.fori_loop(0, 4, put, 0)
        og_copy(i).start()

    @scoped
    def grad_tiles(lo, hi):
        def one(i, carry):
            w_load(i).wait()
            block = dot_nt(og_v[:TOK], w_v[i % W_SLOTS])
            at = pl.ds(pl.multiple_of(i * W_ROWS, W_ROWS), W_ROWS)
            grad_v[:, at] = block

            @pl.when(i + W_SLOTS < W_TILES)
            def _():
                w_load(i + W_SLOTS).start()
            return carry
        lax.fori_loop(lo, hi, one, 0)

    @scoped
    def og_take(i):
        og_copy(i).wait_recv()
        def take(n, carry):
            rows = pl.ds(pl.multiple_of(TOK + n * 64, 64), 64)
            block = parts[i][1, n].reshape(64, WIDTHS[i])
            og_v[rows, STARTS[i]:STARTS[i] + WIDTHS[i]] = block.astype(BF16)
            return carry
        lax.fori_loop(0, 4, take, 0)

    lower = (
        lax.broadcasted_iota(jnp.int32, (TOK, TOK), 0) >= lax.broadcasted_iota(jnp.int32, (TOK, TOK), 1)
    )

    @scoped
    def inside_heads(c):
        def some(js, c):
            at = [cols(4 * j + c) for j in js]
            scores = [dot_nt(q_v[:, a], k_v[:, a]) for a in at]
            probs = [jnp.where(lower, x, 0.0).astype(BF16) for x in scores]
            out = [dot_nn(p, v_v[:, a]) for p, a in zip(probs, at)]
            for a, value in zip(at, out):
                intra_v[:, a] = value
        heads_of(some, c)

    @scoped
    def forward_heads(c):
        def some(js, c):
            at = [cols(4 * j + c) for j in js]
            q = [q_v[:, a] for a in at]
            split = [two_parts(r1[j, c]) for j in js]
            inter = [dot_nn(a, high) + dot_nn(a, low) for a, (high, low) in zip(q, split)]
            o = [intra_v[:, a] + x for a, x in zip(at, inter)]
            inverse = [lax.rsqrt(jnp.mean(x * x, axis=-1, keepdims=True) + EPS) for x in o]
            normed = [x * i for x, i in zip(o, inverse)]
            grad = [grad_v[:, a] for a in at]
            level = [jnp.mean(g * n, axis=-1, keepdims=True) for g, n in zip(grad, normed)]
            d_o = [(i * (g - n * m)).astype(BF16) for i, g, n, m in zip(inverse, grad, normed, level)]
            d_prefix = [dot_tn(a, b) for a, b in zip(q, d_o)]
            att = [n.astype(BF16) for n in normed]
            turned = [a.astype(F32).T.astype(BF16).reshape(2, 4, 16, TOK) for a in att]
            for i, j in enumerate(js):
                h = 4 * j + c
                hh = h % 8
                att_v[:, at[i]] = att[i]
                do_v[:, at[i]] = d_o[i]
                state[j, c] = d_prefix[i]
                attT[h // 8, hh // 2, pl.ds(2 * (hh % 2), 2)] = turned[i]
        heads_of(some, c)

    def att_copies(c):
        return [
            send(attS.at[2 * c + i], attR.at[2 * c + i], ats.at[0], atr.at[c], other)
            for i in range(2)
        ]

    @scoped
    def att_give(c):
        for i, copy in enumerate(att_copies(c)):
            hh = 4 * i + c
            attS[2 * c + i] = attT[1 - d, hh // 2, 2 * (hh % 2):2 * (hh % 2) + 2].astype(F32)
            copy.start()

    @scoped
    def att_take(c):
        both = attR.at[2 * c:2 * c + 2]
        send(both, both, ats.at[0], atr.at[c], other).wait_recv()
        for i in range(2):
            hh = 4 * i + c
            attP[hh // 2, 2 * (hh % 2):2 * (hh % 2) + 2] = attR[2 * c + i].astype(BF16)

    forward = (
        (grad_tiles, 0, 4), (1, 0), (grad_tiles, 4, 6), (1, 1), (grad_tiles, 6, 8), (2, 0), (1, 2),
        (inside_heads, 0), (2, 1), (1, 3), (inside_heads, 1), (3, 0), (2, 2), (og_take, 0), (inside_heads, 2),
        (3, 1), (2, 3), (4, 0), (inside_heads, 3), (3, 2), (4, 1), (3, 3), (og_take, 1), (4, 2), (og_take, 2),
        (4, 3),
    )
    loads[1].wait()
    for item in forward:
        if callable(item[0]):
            item[0](*item[1:])
        else:
            scan1.step(*item)
    scan1.drain(0)
    @scoped
    def product(i, t):
        color = colors[i]
        axis = ORDERS[i][0]
        idx = [slice(None)] * 3
        idx[axis] = t
        idx = tuple(idx)
        both = jnp.concatenate([attT[(d,) + idx].reshape(TOK, TOK), attP[idx].reshape(TOK, TOK)], axis=1)
        for low in range(0, WIDTHS[i], COL):
            high = min(low + COL, WIDTHS[i])
            block = dot_nn(both, og_v[:, STARTS[i] + low:STARTS[i] + high])
            color.part[idx + (slice(None), slice(None), slice(low, high))] = block.reshape(4, 4, 2, 8, high - low)

    @scoped
    def backward_heads(c):
        def some(js, c):
            at = [cols(4 * j + c) for j in js]
            q, k, v, d_o = ([ref[:, a] for a in at] for ref in (q_v, k_v, v_v, do_v))
            probs = [jnp.where(lower, dot_nt(a, b), 0.0).astype(BF16) for a, b in zip(q, k)]
            d_probs = [jnp.where(lower, dot_nt(a, b), 0.0).astype(BF16) for a, b in zip(d_o, v)]
            before = [two_parts(r1[j, c]) for j in js]
            after = [two_parts(r2[j, c]) for j in js]
            n = range(len(js))
            q_grad = [dot_nn(d_probs[i], k[i]) + sum(dot_nt(d_o[i], p) for p in before[i]) for i in n]
            k_grad = [dot_tn(d_probs[i], q[i]) + sum(dot_nt(v[i], p) for p in after[i]) for i in n]
            v_grad = [dot_tn(probs[i], d_o[i]) + sum(dot_nn(k[i], p) for p in after[i]) for i in n]
            for i in n:
                q_v[:, at[i]] = q_grad[i].astype(BF16)
                k_v[:, at[i]] = k_grad[i].astype(BF16)
                v_v[:, at[i]] = v_grad[i].astype(BF16)
        heads_of(some, c)

    cz, cx, cy = colors

    def up_down(color, pair, u):
        color.go(0, 2 * pair, u)
        color.go(0, 2 * pair + 1, u)

    def paced(color, pair, u):
        n = 4 * pair + u - 2
        color.left(n // 4, n % 4)
        up_down(color, pair, u)

    def early_and_late(kinds_even, kinds_odd, us):
        for parity, kinds in ((0, kinds_even), (1, kinds_odd)):
            @pl.when(z % 2 == parity)
            def _(kinds=kinds):
                for u in us:
                    for kind in kinds:
                        cz.go(0, kind, u)

    for c in range(N_CHUNK):
        scan1.step(5, c)
        forward_heads(c)
        scan2.step(0, c)
        att_give(c)
        if c == 2:
            og_copy(0).wait_send()
            att_take(0)
            att_take(1)
            product(0, 0)
            product(0, 2)
            early_and_late((0, 1), (2, 3), (0, 1, 2))
    att_take(2)
    att_take(3)
    for i in (1, 2):
        og_copy(i).wait_send()
    product(1, (x + 2) % 4)
    up_down(cx, 0, 0)
    up_down(cx, 0, 1)
    product(2, (y + 2) % 4)
    for u in range(4):
        up_down(cy, 0, u)
    scan2.step(1, 0)
    product(1, (x + 1) % 4)
    product(1, (x + 3) % 4)
    product(2, (y + 1) % 4)
    product(2, (y + 3) % 4)
    up_down(cy, 1, 0)
    up_down(cy, 1, 1)
    scan2.step(1, 1)
    product(0, 1)
    product(0, 3)
    product(1, x)
    product(2, y)
    scan2.step(1, 2)
    scan2.step(1, 3)
    paced(cx, 0, 2)
    scan2.step(2, 0)
    early_and_late((0, 1), (2, 3), (3,))
    scan2.step(2, 1)
    for stage in range(1, 5):
        scan1.drain(stage)
    paced(cx, 0, 3)
    scan2.step(2, 2)
    early_and_late((2, 3), (0, 1), (0,))
    scan2.step(3, 0)
    paced(cx, 1, 0)
    for item in ((2, 3), (3, 1)):
        scan2.step(*item)
    early_and_late((2, 3), (0, 1), (1, 2, 3))
    paced(cx, 1, 1)
    scan2.step(4, 0)
    scan2.step(3, 2)
    paced(cx, 1, 2)
    paced(cy, 1, 2)
    cz.relay(0, 0)
    scan2.step(4, 1)
    scan2.step(3, 3)
    up_down(cx, 1, 3)
    for u in range(4):
        cx.relay(0, u)
    paced(cy, 1, 3)
    scan2.step(4, 2)
    cy.relay(0, 0)
    scan2.step(4, 3)
    for u in range(1, 4):
        cy.relay(0, u)
    cz.relay(0, 1)
    cz.relay(0, 2)

    def finish_first(color, u):
        color.finish(0, u)
        if u == 0:
            for v in range(4):
                color.go(1, 0, v)
                color.go(1, 1, v)
        elif u < 3:
            color.go(1, 1 + u, 0)

    def finish_second(color, v):
        color.finish(1, v)
        if v < 3:
            color.direct((2, 1, 3)[v]).start()

    for u in range(3):
        scan2.step(5, u)
        backward_heads(u)
        if u == 0:
            cz.relay(0, 3)
    finish_first(cx, 0)
    finish_first(cz, 0)
    scan2.step(5, 3)
    backward_heads(3)
    for color, u in (
        (cx, 1), (cy, 0), (cz, 1), (cx, 2), (cy, 1), (cx, 3), (cz, 2), (cy, 2), (cz, 3), (cy, 3)
    ):
        finish_first(color, u)
    for stage in range(5):
        scan2.drain(stage)
    send(attS, attS, ats.at[0], atr.at[0], other).wait_send()
    for color in colors:
        color.drain(0)
    for v in range(4):
        for color in (cx, cz, cy):
            color.relay(1, v)
            if v < 3:
                color.go(1, 2, v + 1)
                color.go(1, 3, v + 1)
    for v in range(4):
        for color in (cx, cz, cy):
            finish_second(color, v)
    for color in colors:
        color.drain(1)
    for i in (1, 0, 2):
        colors[i].last(wg_v, STARTS[i], WIDTHS[i])
    for color in colors:
        color.drain(2)


def store_kernel(*refs):
    sources, targets, sems = refs[:5], refs[5:10], refs[10]
    copies = [
        pltpu.make_async_copy(src, dst.at[0] if i < 4 else dst, sems.at[i])
        for i, (src, dst) in enumerate(zip(sources, targets))
    ]
    for copy in copies:
        copy.start()
    for copy in copies:
        copy.wait()


def body(queries, keys, values, out_grad, out_weight):
    vm = pltpu.VMEM
    dma = pltpu.SemaphoreType.DMA

    def scan_bufs():
        return [
            vm((4, 4, 128, 128), F32), vm((4, 4, 32, 128), F32), vm((4, 4, 32, 128), F32),
            vm((4, 32, 128), F32), vm((4, 4, 32, 128), F32), vm((4, 4, 32, 128), F32),
            vm((4, 4, 128, 128), F32),
        ]

    scratch = [
        vm((2 * TOK, D), BF16), vm((W_SLOTS, W_ROWS, D), BF16),
        vm((TOK, HD), F32), vm((TOK, HD), F32), vm((TOK, HD), BF16),
        vm((2, 4, 4, 4, 16, TOK), BF16), vm((4, 4, 4, 16, TOK), BF16),
        vm((8, 2, 4, 16, TOK), F32), vm((8, 2, 4, 16, TOK), F32),
        vm((4, 4, 128, 128), F32),
        *scan_bufs(), *scan_bufs(),
        *[vm((4, 4, 4, 2, 8, w), F32) for w in WIDTHS],
    ]
    scratch += [vm((6, 4, 4, 8, w), F32) for w in WIDTHS]
    scratch += [vm((6, 4, 8, w), F32) for w in WIDTHS]
    scratch += [vm((3, 2, 8, w), F32) for w in WIDTHS]
    scratch += [
        dma((4,)), dma((W_SLOTS,)),
        dma((5,)), dma((4, 5)), dma((5,)), dma((4, 5)),
        dma((3, 14)), dma((3, 18)), dma((3,)), dma((3,)), dma((1,)), dma((4,)),
    ]
    any_space = pl.BlockSpec(memory_space=pl.ANY)
    in_vmem = pl.BlockSpec(memory_space=vm)
    results = pl.pallas_call(
        kernel,
        out_shape=(vm((TOK, HD), BF16),) * 4 + (vm((2, 8, D), F32),),
        in_specs=[any_space] * 5,
        out_specs=(in_vmem,) * 5,
        scratch_shapes=scratch,
        compiler_params=pltpu.CompilerParams(
            collective_id=0, has_side_effects=True, vmem_limit_bytes=VMEM_LIMIT
        ),
        name="block",
    )(queries, keys, values, out_grad, out_weight)
    flat = jax.ShapeDtypeStruct((1, TOK, HD), BF16)
    attended, d_query, d_key, d_value, weight_grad = pl.pallas_call(
        store_kernel,
        out_shape=(flat,) * 4 + (jax.ShapeDtypeStruct((2, 8, D), F32),),
        in_specs=[in_vmem] * 5,
        out_specs=(any_space,) * 5,
        scratch_shapes=[dma((5,))],
        compiler_params=pltpu.CompilerParams(vmem_limit_bytes=1 << 20),
        name="store",
    )(*results)
    return attended, d_query, d_key, d_value, weight_grad.reshape(16, D)


def solution(mesh):
    split = Mesh(mesh.devices.reshape(mesh.shape[DP], 4, 4, 4), DP_SEQ)
    rows = P(DP, SEQ, None)
    return jax.shard_map(
        body, mesh=split, in_specs=(rows, rows, rows, rows, P()),
        out_specs=(rows, rows, rows, rows, P(DP_SEQ, None)), check_vma=False,
    )
```
